512 devices in a mesh: dp: 64 (over x, y, z_hi, core), emb: 8 (over z_lo).
Axes of the slice: x: 4, y: 4, z: 16 (z_hi: 2, z_lo: 8; z = z_hi * 8 + z_lo), core: 2. Of those that a mesh axis runs over, the one named last changes fastest.
Arguments:
- cur_ids: int32 [131072], P(('dp', 'emb')), may hold values from 0 to 12287, as said below
- prev_ids: int32 [131072], P(('dp', 'emb')), may hold values from 0 to 12287, as said below
- prev_grads: bfloat16 [131072, 128], P(('dp', 'emb')), may hold values from -6 to 6
- row_place: int32 [12288], replicated, may hold values from 0 to 12287, as said below
- table: float32 [12288, 128], P('emb'), may hold values from -6 to 6
- accum: float32 [12288, 128], P('emb'), may hold values from 0.05 to 2
- labels: float32 [131072], P('dp'), may hold values from 0 to 1
- gain: float32 [128], replicated, may hold values from 0.5 to 1.5
- w_gate: bfloat16 [128, 4096], P(None, 'emb'), may hold values from -0.5 to 0.5
- w_up: bfloat16 [128, 4096], P(None, 'emb'), may hold values from -0.5 to 0.5
- w_out: bfloat16 [4096], P('emb'), may hold values from -0.09375 to 0.09375
Outputs:
- new_table: float32 [12288, 128], P('emb')
- new_accum: float32 [12288, 128], P('emb')
- grad_gate: float32 [128, 4096], P(None, 'emb')
- grad_up: float32 [128, 4096], P(None, 'emb')
- emb_grad: float32 [131072, 128], P(('dp', 'emb'))
The draws below stay inside these ranges and needn't reach their ends.
Inputs may be any that keep to these rules, and one draw needn't show every extreme that they name: A permutation of the table rows; row i is stored on shard row_place[i] // 1536 of emb at position row_place[i] % 1536. `cur_ids`: the 256 ids of one device name rows of one shard at most 64 times, and exactly 64 times for some shard. `prev_ids`: the 256 ids of one device name rows of one shard at most 64 times, and exactly 64 times for some shard.
All inputs are finite; a program needn't handle non-finite values.
Results may differ from the reference program's by a relative error of at most 0.0069.
Values may be sent and summed in bfloat16 or wider, within the bound.
No kernel may reach another device: no remote copies, remote signals or barrier semaphores. Data moves between devices by JAX's collectives and lax.ppermute only.
A program may use at most 64 MiB of HBM per device.

```python
import math
import jax
import jax.numpy as jnp
from jax import lax

E = 128
HID = 4096
TOK_DEV = 256
ROWS_SHARD = 1536
TOKENS = 131072
VOCAB = 12288
CAP = 64
N_DP = 64
N_EMB = 8


def place_table(key):
    return jax.random.permutation(jax.random.fold_in(key, 11), VOCAB).astype(jnp.int32)


def draw_ids(key, salt):
    placement = place_table(key)
    inverse = jnp.zeros((VOCAB,), jnp.int32).at[placement].set(jnp.arange(VOCAB, dtype=jnp.int32))
    blocks = TOKENS // TOK_DEV
    salted = jax.random.fold_in(key, salt)
    hot_shard = jax.random.randint(jax.random.fold_in(salted, 1), (blocks, 1), 0, N_EMB)
    position = jnp.arange(TOK_DEV, dtype=jnp.int32)[None, :]
    others = (hot_shard + 1 + (position - CAP) % max(N_EMB - 1, 1)) % N_EMB
    target = jnp.where(position < CAP, hot_shard, others)
    device_keys = jax.random.split(jax.random.fold_in(salted, 2), blocks)
    shuffle = jax.vmap(lambda one_key: jax.random.permutation(one_key, TOK_DEV))(device_keys)
    target = jnp.take_along_axis(target, shuffle, axis=1)
    first_pick = jax.random.randint(jax.random.fold_in(salted, 3), (blocks, TOK_DEV), 0, ROWS_SHARD)
    second_pick = jax.random.randint(jax.random.fold_in(salted, 4), (blocks, TOK_DEV), 0, ROWS_SHARD)
    slot_index = jnp.minimum(first_pick, second_pick)
    return inverse[target * ROWS_SHARD + slot_index].reshape(TOKENS).astype(jnp.int32)


def draw_row_place(key, part):
    return place_table(key)


def draw_cur_ids(key, part):
    return draw_ids(key, 21)


def draw_prev_ids(key, part):
    return draw_ids(key, 22)


def level_of(key, shape, cuts, smallest, top_value):
    def one(dim, blocks):
        steps = jax.random.uniform(jax.random.fold_in(jax.random.fold_in(key, 6), dim), (blocks,), jnp.float32, smallest / len(cuts), top_value / len(cuts))
        return jnp.repeat(jnp.exp(steps), shape[dim] // blocks).reshape((-1,) + (1,) * (len(shape) - dim - 1))

    factor_of = one(*cuts[0])
    for cut in cuts[1:]:
        factor_of = factor_of * one(*cut)
    return factor_of


def normal_values(rng, dims, deviation, reach, pieces=(), held_as=jnp.bfloat16):
    entries = deviation * jax.random.normal(rng, dims, jnp.float32)
    if pieces:
        entries = entries * level_of(rng, dims, pieces, -0.22, 0.18)
    return jnp.clip(entries, -reach, reach).astype(held_as)


def setup_inputs(seed: int = 0) -> dict:
    key_of = jax.random.split(jax.random.key(seed), 12)
    cur_ids = draw_cur_ids(jax.random.fold_in(key_of[11], 71), 0)
    prev_ids = draw_prev_ids(jax.random.fold_in(key_of[11], 71), 0)
    prev_grads = normal_values(key_of[2], (TOKENS, E), 1.0, 6.0, ((0, 512),))
    row_place = draw_row_place(jax.random.fold_in(key_of[11], 71), 0)
    table = normal_values(key_of[4], (VOCAB, E), 1.0, 6.0, ((0, 8),), jnp.float32)
    accum = jnp.clip(jnp.exp(math.log(2.0) - 3.6888794 * jax.random.uniform(key_of[5], (VOCAB, E), jnp.float32) ** level_of(key_of[5], (VOCAB, E), ((0, 8),), -0.2, 0.2)), 0.05, 2.0)
    labels = jnp.clip(1.0 * jax.random.uniform(key_of[6], (TOKENS,), jnp.float32) ** level_of(key_of[6], (TOKENS,), ((0, 64),), -0.2, 0.2), 0.0, 1.0)
    gain = jnp.clip(1.0 + 0.1 * jax.random.normal(key_of[7], (E,), jnp.float32), 0.5, 1.5)
    w_gate = normal_values(key_of[8], (E, HID), E ** -0.5, 0.5, ((1, 8),))
    w_up = normal_values(key_of[9], (E, HID), E ** -0.5, 0.5, ((1, 8),))
    w_out = normal_values(key_of[10], (HID,), HID ** -0.5, 0.09375, ((0, 8),))
    return {"cur_ids": cur_ids, "prev_ids": prev_ids, "prev_grads": prev_grads, "row_place": row_place, "table": table, "accum": accum, "labels": labels, "gain": gain, "w_gate": w_gate, "w_up": w_up, "w_out": w_out}


loss_weight = 64.0
learn_rate = 0.1
norm_eps = 1e-06

def reference(cur_ids, prev_ids, prev_grads, row_place, table, accum, labels, gain, w_gate, w_up, w_out):
    gain_f = gain.astype(jnp.float32)

    def tower_block(sums_so_far, blocked):
        positions, targets = blocked
        looked_up = table[positions].astype(jnp.bfloat16)
        values = looked_up.astype(jnp.float32)
        inverse_rms = lax.rsqrt(lax.optimization_barrier(jnp.mean(values * values, axis=1, keepdims=True)) + norm_eps)
        normed = (values * inverse_rms * gain_f).astype(jnp.bfloat16)
        gate_proj = jnp.dot(normed, w_gate, preferred_element_type=jnp.float32)
        up_proj = jnp.dot(normed, w_up, preferred_element_type=jnp.float32)
        sigmoid_gate = jax.nn.sigmoid(gate_proj)
        activated = gate_proj * sigmoid_gate
        hidden = (activated * up_proj).astype(jnp.bfloat16)
        logits = jnp.dot(hidden, w_out, preferred_element_type=jnp.float32)
        slopes = loss_weight * (jax.nn.sigmoid(logits) - targets)
        back_hidden = slopes[:, None] * w_out.astype(jnp.float32)[None, :]
        back_gate = (back_hidden * up_proj * sigmoid_gate * (1.0 + gate_proj * (1.0 - sigmoid_gate))).astype(jnp.bfloat16)
        back_up = (back_hidden * activated).astype(jnp.bfloat16)
        contract = (((0,), (0,)), ((), ()))
        gate_part = lax.dot_general(normed, back_gate, contract, preferred_element_type=jnp.float32)
        up_part = lax.dot_general(normed, back_up, contract, preferred_element_type=jnp.float32)
        across = (((1,), (1,)), ((), ()))
        back_normed = lax.dot_general(back_gate, w_gate, across, preferred_element_type=jnp.float32)
        back_normed = back_normed + lax.dot_general(back_up, w_up, across, preferred_element_type=jnp.float32)
        scaled = back_normed * gain_f
        row_grad = inverse_rms * scaled - values * inverse_rms ** 3 * lax.optimization_barrier(jnp.mean(values * scaled, axis=1, keepdims=True))
        return ((sums_so_far[0] + gate_part, sums_so_far[1] + up_part), row_grad)
    positions = row_place[cur_ids].reshape(N_DP, -1)
    targets = labels.reshape(N_DP, -1)
    start_sums = (jnp.zeros((E, HID), jnp.float32), jnp.zeros((E, HID), jnp.float32))
    (gate_sum, up_sum), row_grads = lax.scan(tower_block, start_sums, (positions, targets))
    tower_scale = 1.0 / math.sqrt(TOKENS)
    table_grad = jax.ops.segment_sum(prev_grads.astype(jnp.float32), row_place[prev_ids], num_segments=VOCAB)
    new_accum = accum + table_grad * table_grad
    new_table = table - learn_rate * table_grad * lax.rsqrt(new_accum)
    return (new_table, new_accum, gate_sum * tower_scale, up_sum * tower_scale, row_grads.reshape(TOKENS, E))
```

```python
import math

import jax
import jax.numpy as jnp
from jax import lax
from jax.experimental import pallas as pl
from jax.experimental.pallas import tpu as pltpu
from jax.sharding import Mesh
from jax.sharding import PartitionSpec as P

DP = ("x", "y", "zh", "core")
DP_EMB = ("x", "y", "zh", "core", "emb")
XY = ("x", "y")
ZZ = ("zh", "emb")

loss_weight = 64.0
learn_rate = 0.1
norm_eps = 1e-06

bf16 = jnp.bfloat16
f32 = jnp.float32


def exchange(pieces, axis):
    return lax.all_to_all(pieces, axis, 0, 0, tiled=True)


def to_all(array, axis):
    return exchange(jnp.broadcast_to(array[None], (lax.axis_size(axis), *array.shape)), axis)


def dot32(a, b):
    return jnp.dot(a, b, preferred_element_type=f32)


def placed(ids, row_place):
    lanes = 128
    grid = row_place.reshape(-1, lanes)
    parts = jnp.concatenate([grid // lanes, grid % lanes], axis=1).astype(bf16)
    pick = (ids[:, None] // lanes == jnp.arange(grid.shape[0], dtype=jnp.int32)[None, :]).astype(bf16)
    lines = dot32(pick, parts)
    lane = ids[:, None] % lanes == jnp.arange(lanes, dtype=jnp.int32)[None, :]
    high = jnp.sum(jnp.where(lane, lines[:, :lanes], 0.0), axis=1)
    low = jnp.sum(jnp.where(lane, lines[:, lanes:], 0.0), axis=1)
    return high.astype(jnp.int32) * lanes + low.astype(jnp.int32)


def slots_of(place, rows_shard, capacity, shards):
    owner = place // rows_shard
    slot = place % rows_shard
    match = owner[:, None] == jnp.arange(shards, dtype=jnp.int32)[None, :]
    n = place.shape[0]
    before = (
        jnp.arange(n, dtype=jnp.int32)[:, None] >= jnp.arange(n, dtype=jnp.int32)[None, :]
    ).astype(bf16)
    counts = dot32(before, match.astype(bf16))
    rank = jnp.sum(jnp.where(match, counts, 0.0), axis=1).astype(jnp.int32) - 1
    return slot, owner * capacity + rank


def coded(slot):
    return jnp.stack([slot // 128 + 1, slot % 128], axis=1).astype(bf16)


def code_line(packed, shards, capacity):
    return packed.astype(bf16).reshape(shards, capacity, 2).swapaxes(1, 2).reshape(shards, 1, -1)


def decoded(line, capacity):
    values = line.astype(jnp.int32)
    return ((values[..., :capacity] - 1) * 128 + values[..., capacity:]).reshape(-1)


def tower_kernel(
    answers_ref, target_ref, weights_ref, w_out_ref, gain_ref, labels_ref,
    emb_grad_ref, grads_ref, gate_s, up_s, sig_s,
):
    tok = target_ref.shape[0]
    width = answers_ref.shape[1]
    shards = w_out_ref.shape[0]
    slot_lane = lax.broadcasted_iota(jnp.int32, (tok, answers_ref.shape[0]), 1)
    pick = jnp.where(target_ref[...] == slot_lane, 1.0, 0.0).astype(bf16)
    values = dot32(pick, answers_ref[...])
    inverse_rms = lax.rsqrt(jnp.mean(values * values, axis=1, keepdims=True) + norm_eps)
    gain = gain_ref[...]
    normed = (values * inverse_rms * gain).astype(bf16)
    normed_t = (values * inverse_rms * gain).T.astype(bf16)

    def block(shard, half, side):
        tiles = []
        for tile in (2 * half, 2 * half + 1):
            quarters = [
                weights_ref[side, pl.ds((tile * 4 + k) * shards * 32 + shard * 32, 32), :]
                for k in range(4)
            ]
            tiles.append(jnp.concatenate(quarters, axis=0))
        return jnp.concatenate(tiles, axis=1)

    def forward(shard, total):
        for half in range(2):
            at = shard * 2 + half
            gate = dot32(normed, block(shard, half, 0))
            up = dot32(normed, block(shard, half, 1))
            sig = jax.nn.sigmoid(gate)
            gate_s[at] = gate
            up_s[at] = up
            sig_s[at] = sig
            hidden = (gate * sig * up).astype(bf16).astype(f32)
            for j in range(2):
                out = w_out_ref[shard, pl.ds(2 * half + j, 1), :].astype(f32)
                total = total + hidden[:, j * 128 : (j + 1) * 128] * out
        return total

    total = lax.fori_loop(0, shards, forward, jnp.zeros((tok, 128), f32))
    logits = jnp.sum(total, axis=1, keepdims=True)
    slopes = loss_weight * (jax.nn.sigmoid(logits) - labels_ref[...])

    across = (((1,), (1,)), ((), ()))

    def backward(shard, back):
        for half in range(2):
            at = shard * 2 + half
            gate = gate_s[at]
            up = up_s[at]
            sig = sig_s[at]
            out = jnp.concatenate(
                [w_out_ref[shard, pl.ds(2 * half + j, 1), :].astype(f32) for j in range(2)], axis=1
            )
            back_hidden = slopes * out
            back_gate = (back_hidden * up * sig * (1.0 + gate * (1.0 - sig))).astype(bf16)
            back_up = (back_hidden * (gate * sig)).astype(bf16)
            for side, part in ((0, back_gate), (1, back_up)):
                back = back + lax.dot_general(
                    part, block(shard, half, side), across, preferred_element_type=f32
                )
                grad = dot32(normed_t, part).astype(bf16)
                for j in range(2):
                    tile = 2 * half + j
                    for k in range(4):
                        grads_ref[
                            side, pl.ds((tile * 4 + k) * shards * 32 + shard * 32, 32), :
                        ] = grad[k * 32 : (k + 1) * 32, j * 128 : (j + 1) * 128]
        return back

    back = lax.fori_loop(0, shards, backward, jnp.zeros((tok, width), f32))
    scaled = back * gain
    emb_grad_ref[...] = inverse_rms * scaled - values * (
        inverse_rms * inverse_rms * inverse_rms
    ) * jnp.mean(values * scaled, axis=1, keepdims=True)


def tower(answers, target, weights, w_out, gain, labels):
    tok = target.shape[0]
    width = answers.shape[1]
    shards = w_out.shape[0]
    vmem = pl.BlockSpec(memory_space=pltpu.VMEM)
    return pl.pallas_call(
        tower_kernel,
        out_shape=(
            jax.ShapeDtypeStruct((tok, width), f32),
            jax.ShapeDtypeStruct((2, shards * 512, width), bf16),
        ),
        in_specs=[vmem] * 6,
        out_specs=(vmem, vmem),
        scratch_shapes=[pltpu.VMEM((2 * shards, tok, 256), f32)] * 3,
        compiler_params=pltpu.CompilerParams(vmem_limit_bytes=40 * 1024 * 1024),
        cost_estimate=pl.CostEstimate(
            flops=6 * 2 * tok * width * 4096, bytes_accessed=5 << 20, transcendentals=2 << 20
        ),
        name="tower",
    )(answers, target.reshape(-1, 1), weights, w_out, gain.reshape(1, -1), labels.reshape(-1, 1))


def on_device(
    cur_ids, prev_ids, prev_grads, row_place, table, accum, labels, gain, w_gate, w_up, w_out
):
    shards = lax.axis_size("emb")
    plane = lax.axis_size(XY)
    rows_shard, width = table.shape
    tok = cur_ids.shape[0]
    capacity = min(tok, 2 * tok // shards)
    slots = shards * capacity

    place = placed(jnp.concatenate([cur_ids, prev_ids]), row_place)
    cur_slot, cur_pos = slots_of(place[:tok], rows_shard, capacity, shards)
    prev_slot, prev_pos = slots_of(place[tok:], rows_shard, capacity, shards)
    slot_ids = jnp.arange(slots, dtype=jnp.int32)[:, None]
    cur_pack = (slot_ids == cur_pos[None, :]).astype(bf16)
    prev_pack = (slot_ids == prev_pos[None, :]).astype(bf16)
    cur_codes = code_line(dot32(cur_pack, coded(cur_slot)), shards, capacity)
    prev_codes = code_line(dot32(prev_pack, coded(prev_slot)), shards, capacity)
    prev_rows = dot32(prev_pack, prev_grads).astype(bf16).reshape(shards, capacity, width)

    at = lax.axis_index(XY)
    own_side = jnp.where(lax.axis_index("core") == 0, w_gate, w_up)
    own_slice = lax.dynamic_slice(own_side, ((at % 4) * 32, (at // 4) * 128), (32, 128))
    shared = jnp.concatenate(
        [own_slice, w_out.reshape(4, 128), jnp.zeros((10, 128), bf16)], axis=0
    )
    first = exchange(
        jnp.concatenate(
            [
                prev_rows,
                jnp.broadcast_to(shared[None], (shards, *shared.shape)),
                cur_codes,
                prev_codes,
            ],
            axis=1,
        ),
        "emb",
    )
    got_rows = first[:, :capacity].reshape(slots, width)
    got_slice = first[:, capacity : capacity + 32].reshape(shards * 32, 128)
    all_out = first[:, capacity + 32 : capacity + 36]
    wanted = decoded(first[:, capacity + 46], capacity)
    got_slots = decoded(first[:, capacity + 47], capacity)

    row_ids = jnp.arange(rows_shard, dtype=jnp.int32)
    fetched = dot32(
        (wanted[:, None] == row_ids[None, :]).astype(bf16), table.astype(bf16)
    ).astype(bf16)
    table_grad = dot32((row_ids[:, None] == got_slots[None, :]).astype(bf16), got_rows)

    grad_piece = rows_shard // plane
    second = exchange(
        jnp.concatenate(
            [
                jnp.broadcast_to(got_slice[None], (plane, *got_slice.shape)),
                table_grad.astype(bf16).reshape(plane, grad_piece, width),
            ],
            axis=1,
        ),
        XY,
    )
    answers = exchange(fetched.reshape(shards, capacity, width), "emb").reshape(slots, width)

    lines = plane * shards * 32
    own_weights = second[:, : shards * 32].reshape(lines, 128)
    plane_grad = second[:, shards * 32 :].astype(f32).sum(axis=0).astype(bf16)
    third = exchange(
        jnp.concatenate(
            [
                jnp.broadcast_to(own_weights[None], (2, lines, 128)),
                plane_grad.reshape(2, grad_piece // 2, width),
            ],
            axis=1,
        ),
        "core",
    )
    my_labels = lax.dynamic_slice(labels, (lax.axis_index("emb") * tok,), (tok,))
    emb_grad, tower_grads = tower(answers, cur_pos, third, all_out, gain, my_labels)

    half_grad = third[:, lines:].astype(f32).sum(axis=0)
    half_grad = half_grad + lax.ppermute(half_grad, "zh", [(0, 1), (1, 0)])

    core_sum = exchange(tower_grads, "core").astype(f32).sum(axis=0).astype(bf16)
    fourth = exchange(
        jnp.concatenate(
            [
                core_sum.reshape(plane, shards * 32, 128),
                jnp.broadcast_to(half_grad.astype(bf16)[None], (plane, *half_grad.shape)),
            ],
            axis=1,
        ),
        XY,
    )
    plane_sum = fourth[:, : shards * 32].astype(f32).sum(axis=0).astype(bf16)
    got_grad = fourth[:, shards * 32 :].reshape(rows_shard // 2, width)
    for_z = jnp.broadcast_to(plane_sum.reshape(1, shards, 32, 128), (2, shards, 32, 128))
    tower_sum = exchange(for_z.reshape(2 * shards, 32, 128), ZZ).astype(f32).sum(axis=0)
    side = to_all(tower_sum.astype(bf16), XY).reshape(plane * 32, 128)
    last = to_all(jnp.concatenate([side, got_grad], axis=0), "core")

    tower_scale = 1.0 / math.sqrt(tok * shards * lax.axis_size(DP))
    both = last[:, : plane * 32].astype(f32) * tower_scale
    both = both.reshape(2, 4, 128, 128).swapaxes(1, 2).reshape(2, 128, 512)
    total_grad = (
        last[:, plane * 32 :]
        .reshape(2, plane, grad_piece // 2, width)
        .swapaxes(0, 1)
        .reshape(rows_shard, width)
        .astype(f32)
    )
    new_accum = accum + total_grad * total_grad
    new_table = table - learn_rate * total_grad * lax.rsqrt(new_accum)
    return (new_table, new_accum, both[0], both[1], emb_grad)


def solution(mesh):
    torus = Mesh(mesh.devices.reshape(4, 4, 2, 2, mesh.shape["emb"]), DP_EMB)
    return jax.shard_map(
        on_device,
        mesh=torus,
        in_specs=(
            P(DP_EMB),
            P(DP_EMB),
            P(DP_EMB, None),
            P(),
            P("emb", None),
            P("emb", None),
            P(DP),
            P(),
            P(None, "emb"),
            P(None, "emb"),
            P("emb"),
        ),
        out_specs=(P("emb", None), P("emb", None), P(None, "emb"), P(None, "emb"), P(DP_EMB, None)),
        check_vma=False,
    )
```

```python
import math

import jax
import jax.numpy as jnp
from jax import lax
from jax.experimental import pallas as pl
from jax.experimental.pallas import tpu as pltpu
from jax.sharding import Mesh
from jax.sharding import PartitionSpec as P


DP = ("x", "y", "zh", "core")
DP_EMB = ("x", "y", "zh", "core", "emb")
XY = ("x", "y")
ZZ = ("zh", "emb")

loss_weight = 64.0
learn_rate = 0.1
norm_eps = 1e-06

bf16 = jnp.bfloat16
f32 = jnp.float32


def exchange(pieces, axis):
    return lax.all_to_all(pieces, axis, 0, 0, tiled=True)


def to_all(array, axis):
    return exchange(jnp.broadcast_to(array[None], (lax.axis_size(axis), *array.shape)), axis)


def dot32(a, b):
    return jnp.dot(a, b, preferred_element_type=f32)


def placed(ids, row_place):
    lanes = 128
    grid = row_place.reshape(-1, lanes)
    parts = jnp.concatenate([grid // lanes, grid % lanes], axis=1).astype(bf16)
    pick = (ids[:, None] // lanes == jnp.arange(grid.shape[0], dtype=jnp.int32)[None, :]).astype(bf16)
    lines = dot32(pick, parts)
    lane = ids[:, None] % lanes == jnp.arange(lanes, dtype=jnp.int32)[None, :]
    high = jnp.sum(jnp.where(lane, lines[:, :lanes], 0.0), axis=1)
    low = jnp.sum(jnp.where(lane, lines[:, lanes:], 0.0), axis=1)
    return high.astype(jnp.int32) * lanes + low.astype(jnp.int32)


def slots_of(place, rows_shard, capacity, shards):
    owner = place // rows_shard
    slot = place % rows_shard
    match = owner[:, None] == jnp.arange(shards, dtype=jnp.int32)[None, :]
    n = place.shape[0]
    before = (
        jnp.arange(n, dtype=jnp.int32)[:, None] >= jnp.arange(n, dtype=jnp.int32)[None, :]
    ).astype(bf16)
    counts = dot32(before, match.astype(bf16))
    rank = jnp.sum(jnp.where(match, counts, 0.0), axis=1).astype(jnp.int32) - 1
    return slot, owner * capacity + rank


def coded(slot):
    return jnp.stack([slot // 128 + 1, slot % 128], axis=1).astype(bf16)


def code_line(packed, shards, capacity):
    return packed.astype(bf16).reshape(shards, capacity, 2).swapaxes(1, 2).reshape(shards, 1, -1)


def decoded(line, capacity):
    values = line.astype(jnp.int32)
    return ((values[..., :capacity] - 1) * 128 + values[..., capacity:]).reshape(-1)


def tower_kernel(
    here_ref, answers_ref, target_ref, own_ref, other_ref, w_gate_ref, w_up_ref, w_out_ref,
    gain_ref, labels_ref, emb_grad_ref, grads_ref, weights_s, gate_s, up_s, sig_s,
):
    tok = target_ref.shape[0]
    width = answers_ref.shape[1]
    shards = w_out_ref.shape[0]
    core = here_ref[0]
    home = here_ref[1]
    weights_s[core] = own_ref[...]
    weights_s[1 - core] = other_ref[...]
    slot_lane = lax.broadcasted_iota(jnp.int32, (tok, answers_ref.shape[0]), 1)
    pick = jnp.where(target_ref[...] == slot_lane, 1.0, 0.0).astype(bf16)
    values = dot32(pick, answers_ref[...])
    inverse_rms = lax.rsqrt(jnp.mean(values * values, axis=1, keepdims=True) + norm_eps)
    gain = gain_ref[...]
    normed_wide = values * inverse_rms * gain
    normed = normed_wide.astype(bf16)
    normed_t = normed_wide.T.astype(bf16)

    def far_block(hop, half, side):
        tiles = []
        for tile in (2 * half, 2 * half + 1):
            quarters = [
                weights_s[side, pl.ds((tile * 4 + k) * (shards - 1) * 32 + hop * 32, 32), :]
                for k in range(4)
            ]
            tiles.append(jnp.concatenate(quarters, axis=0))
        return jnp.concatenate(tiles, axis=1)

    def home_block(hop, half, side):
        return (w_gate_ref, w_up_ref)[side][:, half * 256 : (half + 1) * 256]

    def out_row(shard, half, j):
        return w_out_ref[shard, pl.ds(2 * half + j, 1), :].astype(f32)

    def forward(hop, total, block):
        shard = (home + 1 + hop) % shards
        for half in range(2):
            at = hop * 2 + half
            gate = dot32(normed, block(hop, half, 0))
            up = dot32(normed, block(hop, half, 1))
            sig = jax.nn.sigmoid(gate)
            gate_s[at] = gate
            up_s[at] = up
            sig_s[at] = sig
            hidden = (gate * sig * up).astype(bf16).astype(f32)
            for j in range(2):
                total = total + hidden[:, j * 128 : (j + 1) * 128] * out_row(shard, half, j)
        return total

    total = forward(shards - 1, jnp.zeros((tok, 128), f32), home_block)
    total = lax.fori_loop(0, shards - 1, lambda hop, t: forward(hop, t, far_block), total)
    logits = jnp.sum(total, axis=1, keepdims=True)
    slopes = loss_weight * (jax.nn.sigmoid(logits) - labels_ref[...])

    across = (((1,), (1,)), ((), ()))

    def backward(hop, back, block):
        shard = (home + 1 + hop) % shards
        for half in range(2):
            at = hop * 2 + half
            gate = gate_s[at]
            up = up_s[at]
            sig = sig_s[at]
            out = jnp.concatenate([out_row(shard, half, j) for j in range(2)], axis=1)
            back_hidden = slopes * out
            back_gate = (back_hidden * up * sig * (1.0 + gate * (1.0 - sig))).astype(bf16)
            back_up = (back_hidden * (gate * sig)).astype(bf16)
            for side, part in ((0, back_gate), (1, back_up)):
                back = back + lax.dot_general(
                    part, block(hop, half, side), across, preferred_element_type=f32
                )
                grad = dot32(normed_t, part).astype(bf16)
                place = core if side == 0 else 1 - core
                for j in range(2):
                    tile = 2 * half + j
                    for k in range(4):
                        grads_ref[
                            place, pl.ds((tile * 4 + k) * shards * 32 + shard * 32, 32), :
                        ] = grad[k * 32 : (k + 1) * 32, j * 128 : (j + 1) * 128]
        return back

    back = backward(shards - 1, jnp.zeros((tok, width), f32), home_block)
    back = lax.fori_loop(0, shards - 1, lambda hop, b: backward(hop, b, far_block), back)
    scaled = back * gain
    emb_grad_ref[...] = inverse_rms * scaled - values * (
        inverse_rms * inverse_rms * inverse_rms
    ) * jnp.mean(values * scaled, axis=1, keepdims=True)


def tower(here, answers, target, own, other, w_gate, w_up, w_out, gain, labels):
    tok = target.shape[0]
    width = answers.shape[1]
    shards = w_out.shape[0]
    vmem = pl.BlockSpec(memory_space=pltpu.VMEM)
    return pl.pallas_call(
        tower_kernel,
        out_shape=(
            jax.ShapeDtypeStruct((tok, width), f32),
            jax.ShapeDtypeStruct((2, shards * 512, width), bf16),
        ),
        in_specs=[pl.BlockSpec(memory_space=pltpu.SMEM)] + [vmem] * 9,
        out_specs=(vmem, vmem),
        scratch_shapes=[pltpu.VMEM((2, *own.shape), bf16)]
        + [pltpu.VMEM((2 * shards, tok, 256), f32)] * 3,
        compiler_params=pltpu.CompilerParams(vmem_limit_bytes=24 * 1024 * 1024),
        cost_estimate=pl.CostEstimate(
            flops=6 * 2 * tok * width * 4096, bytes_accessed=5 << 20, transcendentals=2 << 20
        ),
        name="tower",
    )(
        here, answers, target.reshape(-1, 1), own, other, w_gate, w_up, w_out,
        gain.reshape(1, -1), labels.reshape(-1, 1),
    )


def update_kernel(
    here_ref, own_ref, other_ref, table_ref, accum_ref,
    new_table_ref, new_accum_ref, gate_ref, up_ref, both_s, *, scale,
):
    core = here_ref[0]
    both_s[core] = own_ref[...]
    both_s[1 - core] = other_ref[...]
    plane, lines = own_ref.shape[:2]
    span = lines - 32
    for side, out_ref in ((0, gate_ref), (1, up_ref)):
        for q in range(plane):
            tile, k = q // 4, q % 4
            out_ref[k * 32 : (k + 1) * 32, tile * 128 : (tile + 1) * 128] = (
                both_s[side, q, :32, :].astype(f32) * scale
            )
            rows = pl.ds((2 * q + side) * span, span)
            grad = both_s[side, q, 32:, :].astype(f32)
            total = accum_ref[rows, :] + grad * grad
            new_accum_ref[rows, :] = total
            new_table_ref[rows, :] = table_ref[rows, :] - learn_rate * grad * lax.rsqrt(total)


def update(here, own, other, table, accum, scale):
    vmem = pl.BlockSpec(memory_space=pltpu.VMEM)
    part = jax.ShapeDtypeStruct((128, 512), f32)
    return pl.pallas_call(
        lambda *refs: update_kernel(*refs, scale=scale),
        out_shape=(
            jax.ShapeDtypeStruct(table.shape, f32),
            jax.ShapeDtypeStruct(table.shape, f32),
            part,
            part,
        ),
        in_specs=[pl.BlockSpec(memory_space=pltpu.SMEM)] + [vmem] * 4,
        out_specs=(vmem,) * 4,
        scratch_shapes=[pltpu.VMEM((2, *own.shape), bf16)],
        compiler_params=pltpu.CompilerParams(vmem_limit_bytes=12 * 1024 * 1024),
        name="update",
    )(here, own, other, table, accum)


def swapped(array, axis):
    return lax.ppermute(array, axis, [(0, 1), (1, 0)])


def step(
    cur_ids, prev_ids, prev_grads, row_place, table, accum, labels, gain, w_gate, w_up, w_out
):
    shards = lax.axis_size("emb")
    plane = lax.axis_size(XY)
    rows_shard, width = table.shape
    tok = cur_ids.shape[0]
    capacity = min(tok, 2 * tok // shards)
    slots = shards * capacity
    core = lax.axis_index("core")
    home = lax.axis_index("emb")
    here = jnp.stack([core, home]).astype(jnp.int32)

    cur_slot, cur_pos = slots_of(placed(cur_ids, row_place), rows_shard, capacity, shards)
    prev_slot, prev_pos = slots_of(placed(prev_ids, row_place), rows_shard, capacity, shards)
    slot_ids = jnp.arange(slots, dtype=jnp.int32)[:, None]
    cur_pack = (slot_ids == cur_pos[None, :]).astype(bf16)
    prev_pack = (slot_ids == prev_pos[None, :]).astype(bf16)
    cur_codes = code_line(dot32(cur_pack, coded(cur_slot)), shards, capacity)
    prev_codes = code_line(dot32(prev_pack, coded(prev_slot)), shards, capacity)
    prev_rows = dot32(prev_pack, prev_grads).astype(bf16).reshape(shards, capacity, width)

    at = lax.axis_index(XY)
    own_side = jnp.where(core == 0, w_gate, w_up)
    own_slice = lax.dynamic_slice(own_side, ((at % 4) * 32, (at // 4) * 128), (32, 128))
    shared = jnp.concatenate(
        [own_slice, w_out.reshape(4, 128), jnp.zeros((10, 128), bf16)], axis=0
    )
    first = exchange(
        jnp.concatenate(
            [
                prev_rows,
                jnp.broadcast_to(shared[None], (shards, *shared.shape)),
                cur_codes,
                prev_codes,
            ],
            axis=1,
        ),
        "emb",
    )
    got_rows = first[:, :capacity].reshape(slots, width)
    slices = first[:, capacity : capacity + 32]
    all_out = first[:, capacity + 32 : capacity + 36]
    wanted = decoded(first[:, capacity + 46], capacity)
    got_slots = decoded(first[:, capacity + 47], capacity)

    row_ids = jnp.arange(rows_shard, dtype=jnp.int32)
    fetched = dot32(
        (wanted[:, None] == row_ids[None, :]).astype(bf16), table.astype(bf16)
    ).astype(bf16)
    answers = exchange(fetched.reshape(shards, capacity, width), "emb").reshape(slots, width)

    foreign = lax.dynamic_slice(
        jnp.concatenate([slices, slices], axis=0), (home + 1, 0, 0), (shards - 1, 32, 128)
    ).reshape((shards - 1) * 32, 128)
    own_weights = lax.all_gather(foreign, XY, axis=0, tiled=True)
    other_weights = swapped(own_weights, "core")

    table_grad = dot32((row_ids[:, None] == got_slots[None, :]).astype(bf16), got_rows)
    span = rows_shard // plane // 2
    pieces = table_grad.reshape(plane, 2, span, width)
    mine = lax.dynamic_index_in_dim(pieces, core, 1, keepdims=False)
    theirs = lax.dynamic_index_in_dim(pieces, 1 - core, 1, keepdims=False)
    pair_grad = (mine + swapped(theirs, "core")).astype(bf16)

    answers, pair_grad = lax.optimization_barrier((answers, pair_grad))
    my_labels = lax.dynamic_slice(labels, (home * tok,), (tok,))
    emb_grad, tower_grads = tower(
        here, answers, cur_pos, own_weights, other_weights, w_gate, w_up, all_out, gain, my_labels
    )

    received = swapped(tower_grads[1], "core")
    core_sum = (tower_grads[0].astype(f32) + received.astype(f32)).astype(bf16)
    second = exchange(
        jnp.concatenate([core_sum.reshape(plane, shards * 32, 128), pair_grad], axis=1), XY
    )
    plane_sum = second[:, : shards * 32].astype(f32).sum(axis=0).astype(bf16)
    half_grad = second[:, shards * 32 :].astype(f32).sum(axis=0)
    for_z = jnp.broadcast_to(plane_sum.reshape(1, shards, 32, 128), (2, shards, 32, 128))
    third = exchange(for_z.reshape(2 * shards, 32, 128), ZZ)
    tower_sum = third.astype(f32).sum(axis=0).astype(bf16)
    total_grad = (half_grad + swapped(half_grad, "zh")).astype(bf16)
    own = to_all(jnp.concatenate([tower_sum, total_grad], axis=0), XY)
    other = swapped(own, "core")

    tower_scale = 1.0 / math.sqrt(tok * shards * lax.axis_size(DP))
    new_table, new_accum, gate_sum, up_sum = update(here, own, other, table, accum, tower_scale)
    return (new_table, new_accum, gate_sum, up_sum, emb_grad)


def solution(mesh):
    torus = Mesh(mesh.devices.reshape(4, 4, 2, 2, mesh.shape["emb"]), DP_EMB)
    return jax.shard_map(
        step,
        mesh=torus,
        in_specs=(
            P(DP_EMB),
            P(DP_EMB),
            P(DP_EMB, None),
            P(),
            P("emb", None),
            P("emb", None),
            P(DP),
            P(),
            P(None, "emb"),
            P(None, "emb"),
            P("emb"),
        ),
        out_specs=(P("emb", None), P("emb", None), P(None, "emb"), P(None, "emb"), P(DP_EMB, None)),
        check_vma=False,
    )
```

```python
import math

import jax
import jax.numpy as jnp
from jax import lax
from jax.experimental import pallas as pl
from jax.experimental.pallas import tpu as pltpu
from jax.sharding import Mesh
from jax.sharding import PartitionSpec as P


DP = ("x", "y", "zh", "core")
DP_EMB = ("x", "y", "zh", "core", "emb")
XY = ("x", "y")
ZZ = ("zh", "emb")

loss_weight = 64.0
learn_rate = 0.1
norm_eps = 1e-06

bf16 = jnp.bfloat16
f32 = jnp.float32


def exchange(pieces, axis):
    return lax.all_to_all(pieces, axis, 0, 0, tiled=True)


def to_all(array, axis):
    return exchange(jnp.broadcast_to(array[None], (lax.axis_size(axis), *array.shape)), axis)


def dot32(a, b):
    return jnp.dot(a, b, preferred_element_type=f32)


def packed(ids, parts, capacity, shards, rows_shard):
    tok = ids.shape[1]
    lines = parts.shape[0]
    row = lax.broadcasted_iota(jnp.int32, (lines, tok), 0)
    pick = jnp.where(ids // 128 == row, 1.0, 0.0).astype(bf16)
    found = lax.dot_general(parts, pick, (((0,), (0,)), ((), ())), preferred_element_type=f32)
    lane = lax.broadcasted_iota(jnp.int32, (128, tok), 0) == ids % 128
    high = jnp.sum(jnp.where(lane, found[:128], 0.0), axis=0, keepdims=True)
    low = jnp.sum(jnp.where(lane, found[128:], 0.0), axis=0, keepdims=True)
    place = (high * 128.0 + low).astype(jnp.int32)
    shard = lax.broadcasted_iota(jnp.int32, (shards, tok), 0)
    match = (place >= shard * rows_shard) & (place < (shard + 1) * rows_shard)
    matched = jnp.where(match, 1.0, 0.0)
    owner = jnp.sum(jnp.where(match, shard, 0), axis=0, keepdims=True)
    slot = place - owner * rows_shard
    earlier = lax.broadcasted_iota(jnp.int32, (tok, tok), 0) <= lax.broadcasted_iota(
        jnp.int32, (tok, tok), 1
    )
    counts = dot32(matched.astype(bf16), jnp.where(earlier, 1.0, 0.0).astype(bf16))
    rank = jnp.sum(matched * counts, axis=0, keepdims=True).astype(jnp.int32) - 1
    line = lax.broadcasted_iota(jnp.int32, (128, tok), 0)
    spread = jnp.where(line % capacity == rank, 1.0, 0.0).astype(bf16)
    both = (((1,), (1,)), ((), ()))
    codes = [
        lax.dot_general(
            (matched * part.astype(f32)).astype(bf16), spread, both, preferred_element_type=f32
        )
        for part in (slot // 128 + 1, slot % 128)
    ]
    first_half = lax.broadcasted_iota(jnp.int32, (shards, 128), 1) < capacity
    code = jnp.where(first_half, codes[0], codes[1])
    return code, owner * capacity + rank


def pack_kernel(
    here_ref, *refs, capacity, rows_shard
):
    sources, (out_ref, pos_ref), buffers, sems = refs[:7], refs[7:9], refs[9:16], refs[16]
    copies = [
        pltpu.make_async_copy(source, buffer, sems.at[i])
        for i, (source, buffer) in enumerate(zip(sources, buffers, strict=True))
    ]
    for copy in copies:
        copy.start()
    for copy in copies:
        copy.wait()
    cur_ref, prev_ref, grads_ref, places_ref, w_gate_ref, w_up_ref, w_out_ref = buffers
    shards = out_ref.shape[0]
    places = places_ref[...]
    parts = jnp.concatenate(
        [(places // 128).astype(f32), (places % 128).astype(f32)], axis=1
    ).astype(bf16)
    cur_code, cur_pos = packed(cur_ref[...], parts, capacity, shards, rows_shard)
    prev_code, prev_pos = packed(prev_ref[...], parts, capacity, shards, rows_shard)
    pos_ref[...] = cur_pos
    slots = shards * capacity
    slot_row = lax.broadcasted_iota(jnp.int32, (slots, prev_pos.shape[1]), 0)
    pack = jnp.where(slot_row == prev_pos, 1.0, 0.0).astype(bf16)
    rows = dot32(pack, grads_ref[...]).astype(bf16)
    at = here_ref[2]
    cut = (pl.ds(pl.multiple_of((at % 4) * 32, 32), 32), pl.ds(pl.multiple_of((at // 4) * 128, 128), 128))
    gate_slice = w_gate_ref[cut].astype(f32)
    up_slice = w_up_ref[cut].astype(f32)
    own = jnp.where(here_ref[0] == 0, gate_slice, up_slice).astype(bf16)
    out = jnp.concatenate([w_out_ref[...].astype(f32), jnp.zeros((12, 128), f32)], axis=0)
    tail_row = lax.broadcasted_iota(jnp.int32, (16, 128), 0)
    for shard in range(shards):
        out_ref[shard, :capacity, :] = rows[shard * capacity : (shard + 1) * capacity]
        out_ref[shard, capacity : capacity + 32, :] = own
        tail = jnp.where(tail_row == 14, cur_code[shard : shard + 1], out)
        tail = jnp.where(tail_row == 15, prev_code[shard : shard + 1], tail)
        out_ref[shard, capacity + 32 : capacity + 48, :] = tail.astype(bf16)


def pack(here, cur_ids, prev_ids, prev_grads, row_place, w_gate, w_up, w_out, shards, capacity, rows_shard):
    vmem = pl.BlockSpec(memory_space=pltpu.VMEM)
    tok = cur_ids.shape[0]
    arrays = (
        cur_ids.reshape(1, tok), prev_ids.reshape(1, tok), prev_grads,
        row_place.reshape(-1, 128), w_gate, w_up, w_out.reshape(4, 128),
    )
    return pl.pallas_call(
        lambda *refs: pack_kernel(*refs, capacity=capacity, rows_shard=rows_shard),
        out_shape=(
            jax.ShapeDtypeStruct((shards, capacity + 48, 128), bf16),
            jax.ShapeDtypeStruct((1, tok), jnp.int32),
        ),
        in_specs=[pl.BlockSpec(memory_space=pltpu.SMEM)]
        + [pl.BlockSpec(memory_space=pltpu.HBM)] * len(arrays),
        out_specs=(vmem, vmem),
        scratch_shapes=[pltpu.VMEM(array.shape, array.dtype) for array in arrays]
        + [pltpu.SemaphoreType.DMA((len(arrays),))],
        compiler_params=pltpu.CompilerParams(vmem_limit_bytes=62 * 1024 * 1024),
        name="pack",
    )(here, *arrays)


def decoded(line, capacity):
    values = line.astype(jnp.int32)
    return ((values[..., :capacity] - 1) * 128 + values[..., capacity:]).reshape(-1)


def tower_kernel(
    here_ref, answers_ref, target_ref, own_ref, other_ref, w_gate_ref, w_up_ref, shared_ref,
    gain_ref, labels_ref, emb_grad_ref, grads_ref, weights_s, gate_s, up_s, sig_s,
):
    tok = target_ref.shape[1]
    width = answers_ref.shape[1]
    shards, span = shared_ref.shape[:2]
    lines = own_ref.shape[0] // 16
    core = here_ref[0]
    home = here_ref[1]
    weights_s[core] = own_ref[...]
    weights_s[1 - core] = other_ref[...]
    slot_row = lax.broadcasted_iota(jnp.int32, (answers_ref.shape[0], tok), 0)
    pick = jnp.where(target_ref[...] == slot_row, 1.0, 0.0).astype(bf16)
    values = lax.dot_general(
        pick, answers_ref[...], (((0,), (0,)), ((), ())), preferred_element_type=f32
    )
    turned = labels_ref[...].T
    column = lax.broadcasted_iota(jnp.int32, turned.shape, 1) == home
    targets = jnp.sum(jnp.where(column, turned, 0.0), axis=1, keepdims=True)
    inverse_rms = lax.rsqrt(jnp.mean(values * values, axis=1, keepdims=True) + norm_eps)
    gain = gain_ref[...]
    normed_wide = values * inverse_rms * gain
    normed = normed_wide.astype(bf16)
    normed_t = normed_wide.T.astype(bf16)

    def far_block(hop, half, side):
        tiles = []
        for tile in (2 * half, 2 * half + 1):
            quarters = [
                weights_s[side, pl.ds((tile * 4 + k) * lines + hop * 32, 32), :]
                for k in range(4)
            ]
            tiles.append(jnp.concatenate(quarters, axis=0))
        return jnp.concatenate(tiles, axis=1)

    def home_block(hop, half, side):
        return (w_gate_ref, w_up_ref)[side][:, half * 256 : (half + 1) * 256]

    def out_row(shard, half, j):
        return shared_ref[shard, pl.ds(span - 16 + 2 * half + j, 1), :].astype(f32)

    def forward(hop, total, block):
        shard = (home + 1 + hop) % shards
        for half in range(2):
            at = hop * 2 + half
            gate = dot32(normed, block(hop, half, 0))
            up = dot32(normed, block(hop, half, 1))
            sig = jax.nn.sigmoid(gate)
            gate_s[at] = gate
            up_s[at] = up
            sig_s[at] = sig
            hidden = (gate * sig * up).astype(bf16).astype(f32)
            for j in range(2):
                total = total + hidden[:, j * 128 : (j + 1) * 128] * out_row(shard, half, j)
        return total

    total = forward(shards - 1, jnp.zeros((tok, 128), f32), home_block)
    total = lax.fori_loop(0, shards - 1, lambda hop, t: forward(hop, t, far_block), total)
    logits = jnp.sum(total, axis=1, keepdims=True)
    slopes = loss_weight * (jax.nn.sigmoid(logits) - targets)

    across = (((1,), (1,)), ((), ()))

    def backward(hop, back, block):
        shard = (home + 1 + hop) % shards
        for half in range(2):
            at = hop * 2 + half
            gate = gate_s[at]
            up = up_s[at]
            sig = sig_s[at]
            out = jnp.concatenate([out_row(shard, half, j) for j in range(2)], axis=1)
            back_hidden = slopes * out
            back_gate = (back_hidden * up * sig * (1.0 + gate * (1.0 - sig))).astype(bf16)
            back_up = (back_hidden * (gate * sig)).astype(bf16)
            for side, part in ((0, back_gate), (1, back_up)):
                back = back + lax.dot_general(
                    part, block(hop, half, side), across, preferred_element_type=f32
                )
                grad = dot32(normed_t, part).astype(bf16)
                place = core if side == 0 else 1 - core
                for j in range(2):
                    tile = 2 * half + j
                    for k in range(4):
                        grads_ref[
                            place, pl.ds((tile * 4 + k) * shards * 32 + shard * 32, 32), :
                        ] = grad[k * 32 : (k + 1) * 32, j * 128 : (j + 1) * 128]
        return back

    back = backward(shards - 1, jnp.zeros((tok, width), f32), home_block)
    back = lax.fori_loop(0, shards - 1, lambda hop, b: backward(hop, b, far_block), back)
    scaled = back * gain
    emb_grad_ref[...] = inverse_rms * scaled - values * (
        inverse_rms * inverse_rms * inverse_rms
    ) * jnp.mean(values * scaled, axis=1, keepdims=True)


def tower(here, answers, target, own, other, w_gate, w_up, shared, gain, labels):
    tok = target.shape[1]
    width = answers.shape[1]
    shards = shared.shape[0]
    vmem = pl.BlockSpec(memory_space=pltpu.VMEM)
    return pl.pallas_call(
        tower_kernel,
        out_shape=(
            jax.ShapeDtypeStruct((tok, width), f32),
            jax.ShapeDtypeStruct((2, shards * 512, width), bf16),
        ),
        in_specs=[pl.BlockSpec(memory_space=pltpu.SMEM)] + [vmem] * 9,
        out_specs=(vmem, vmem),
        scratch_shapes=[pltpu.VMEM((2, *own.shape), bf16)]
        + [pltpu.VMEM((2 * shards, tok, 256), f32)] * 3,
        compiler_params=pltpu.CompilerParams(vmem_limit_bytes=24 * 1024 * 1024),
        cost_estimate=pl.CostEstimate(
            flops=6 * 2 * tok * width * 4096, bytes_accessed=5 << 20, transcendentals=2 << 20
        ),
        name="tower",
    )(
        here, answers, target, own, other, w_gate, w_up, shared,
        gain.reshape(1, -1), labels.reshape(shards, tok),
    )


def update_kernel(
    here_ref, own_ref, other_ref, table_ref, accum_ref,
    new_table_ref, new_accum_ref, gate_ref, up_ref, both_s, *, scale,
):
    core = here_ref[0]
    both_s[core] = own_ref[...]
    both_s[1 - core] = other_ref[...]
    plane, lines = own_ref.shape[:2]
    span = lines - 32
    for side, out_ref in ((0, gate_ref), (1, up_ref)):
        for q in range(plane):
            tile, k = q // 4, q % 4
            out_ref[k * 32 : (k + 1) * 32, tile * 128 : (tile + 1) * 128] = (
                both_s[side, q, :32, :].astype(f32) * scale
            )
            rows = pl.ds((2 * q + side) * span, span)
            grad = both_s[side, q, 32:, :].astype(f32)
            total = accum_ref[rows, :] + grad * grad
            new_accum_ref[rows, :] = total
            new_table_ref[rows, :] = table_ref[rows, :] - learn_rate * grad * lax.rsqrt(total)


def update(here, own, other, table, accum, scale):
    vmem = pl.BlockSpec(memory_space=pltpu.VMEM)
    part = jax.ShapeDtypeStruct((128, 512), f32)
    return pl.pallas_call(
        lambda *refs: update_kernel(*refs, scale=scale),
        out_shape=(
            jax.ShapeDtypeStruct(table.shape, f32),
            jax.ShapeDtypeStruct(table.shape, f32),
            part,
            part,
        ),
        in_specs=[pl.BlockSpec(memory_space=pltpu.SMEM)] + [vmem] * 4,
        out_specs=(vmem,) * 4,
        scratch_shapes=[pltpu.VMEM((2, *own.shape), bf16)],
        compiler_params=pltpu.CompilerParams(vmem_limit_bytes=12 * 1024 * 1024),
        name="update",
    )(here, own, other, table, accum)


def swapped(array, axis):
    return lax.ppermute(array, axis, [(0, 1), (1, 0)])


def step(
    cur_ids, prev_ids, prev_grads, row_place, table, accum, labels, gain, w_gate, w_up, w_out
):
    shards = lax.axis_size("emb")
    plane = lax.axis_size(XY)
    rows_shard, width = table.shape
    tok = cur_ids.shape[0]
    capacity = min(tok, 2 * tok // shards)
    slots = shards * capacity
    core = lax.axis_index("core")
    home = lax.axis_index("emb")
    here = jnp.stack([core, home, lax.axis_index(XY)]).astype(jnp.int32)

    payload, cur_pos = pack(
        here, cur_ids, prev_ids, prev_grads, row_place, w_gate, w_up, w_out,
        shards, capacity, rows_shard,
    )
    first = exchange(payload, "emb")
    got_rows = first[:, :capacity].reshape(slots, width)
    slices = first[:, capacity : capacity + 32]
    wanted = decoded(first[:, capacity + 46], capacity)
    got_slots = decoded(first[:, capacity + 47], capacity)

    row_ids = jnp.arange(rows_shard, dtype=jnp.int32)
    fetched = dot32(
        (wanted[:, None] == row_ids[None, :]).astype(bf16), table.astype(bf16)
    ).astype(bf16)
    answers = exchange(fetched.reshape(shards, capacity, width), "emb").reshape(slots, width)

    span = rows_shard // plane // 2
    half_ids = jnp.arange(rows_shard // 2, dtype=jnp.int32)
    half_ids = half_ids // span * (2 * span) + half_ids % span

    def half_sum(side):
        hot = (half_ids + side * span)[:, None] == got_slots[None, :]
        return dot32(hot.astype(bf16), got_rows).reshape(plane, span, width)

    received = swapped(half_sum(1 - core), "core")
    pair_grad = (half_sum(core) + received).astype(bf16)

    foreign = lax.dynamic_slice(
        jnp.concatenate([slices, slices], axis=0), (home + 1, 0, 0), (shards - 1, 32, 128)
    ).reshape((shards - 1) * 32, 128)
    lines = foreign.shape[0]
    plane_in = jnp.concatenate(
        [jnp.broadcast_to(foreign[None], (plane, *foreign.shape)), pair_grad], axis=1
    )
    answers, plane_in = lax.optimization_barrier((answers, plane_in))
    planes = exchange(plane_in, XY)
    own_weights = planes.reshape(-1, 128)
    other_weights = swapped(own_weights, "core")
    half_grad = planes[:, lines:].astype(f32).sum(axis=0)

    emb_grad, tower_grads = tower(
        here, answers, cur_pos, own_weights, other_weights, w_gate, w_up, first, gain, labels
    )

    received = swapped(tower_grads[1], "core")
    core_sum = (tower_grads[0].astype(f32) + received.astype(f32)).astype(bf16)
    second = exchange(core_sum.reshape(plane, shards * 32, 128), XY)
    total_grad = (half_grad + swapped(half_grad, "zh")).astype(bf16)
    second, total_grad = lax.optimization_barrier((second, total_grad))
    plane_sum = second.astype(f32).sum(axis=0).astype(bf16)
    for_z = jnp.broadcast_to(plane_sum.reshape(1, shards, 32, 128), (2, shards, 32, 128))
    third = exchange(for_z.reshape(2 * shards, 32, 128), ZZ)
    tower_sum = third.astype(f32).sum(axis=0).astype(bf16)
    own = to_all(jnp.concatenate([tower_sum, total_grad], axis=0), XY)
    other = swapped(own, "core")

    tower_scale = 1.0 / math.sqrt(tok * shards * lax.axis_size(DP))
    new_table, new_accum, gate_sum, up_sum = update(here, own, other, table, accum, tower_scale)
    return (new_table, new_accum, gate_sum, up_sum, emb_grad)


def solution(mesh):
    torus = Mesh(mesh.devices.reshape(4, 4, 2, 2, mesh.shape["emb"]), DP_EMB)
    return jax.shard_map(
        step,
        mesh=torus,
        in_specs=(
            P(DP_EMB),
            P(DP_EMB),
            P(DP_EMB, None),
            P(),
            P("emb", None),
            P("emb", None),
            P(DP),
            P(),
            P(None, "emb"),
            P(None, "emb"),
            P("emb"),
        ),
        out_specs=(P("emb", None), P("emb", None), P(None, "emb"), P(None, "emb"), P(DP_EMB, None)),
        check_vma=False,
    )
```

```python
import math

import jax
import jax.numpy as jnp
from jax import lax
from jax.experimental import pallas as pl
from jax.experimental.pallas import tpu as pltpu
from jax.sharding import Mesh
from jax.sharding import PartitionSpec as P


DP = ("x", "y", "zh", "core")
DP_EMB = ("x", "y", "zh", "core", "emb")
XY = ("x", "y")
ZZ = ("zh", "emb")

loss_weight = 64.0
learn_rate = 0.1
norm_eps = 1e-06

bf16 = jnp.bfloat16
f32 = jnp.float32


def exchange(pieces, axis):
    return lax.all_to_all(pieces, axis, 0, 0, tiled=True)


def to_all(array, axis):
    return exchange(jnp.broadcast_to(array[None], (lax.axis_size(axis), *array.shape)), axis)


def dot32(a, b):
    return jnp.dot(a, b, preferred_element_type=f32)


def packed(ids, parts, capacity, shards, rows_shard):
    tok = ids.shape[1]
    lines = parts.shape[0]
    row = lax.broadcasted_iota(jnp.int32, (lines, tok), 0)
    pick = jnp.where(ids // 128 == row, 1.0, 0.0).astype(bf16)
    found = lax.dot_general(parts, pick, (((0,), (0,)), ((), ())), preferred_element_type=f32)
    lane = lax.broadcasted_iota(jnp.int32, (128, tok), 0) == ids % 128
    high = jnp.sum(jnp.where(lane, found[:128], 0.0), axis=0, keepdims=True)
    low = jnp.sum(jnp.where(lane, found[128:], 0.0), axis=0, keepdims=True)
    place = (high * 128.0 + low).astype(jnp.int32)
    shard = lax.broadcasted_iota(jnp.int32, (shards, tok), 0)
    match = (place >= shard * rows_shard) & (place < (shard + 1) * rows_shard)
    matched = jnp.where(match, 1.0, 0.0)
    owner = jnp.sum(jnp.where(match, shard, 0), axis=0, keepdims=True)
    slot = place - owner * rows_shard
    earlier = lax.broadcasted_iota(jnp.int32, (tok, tok), 0) <= lax.broadcasted_iota(
        jnp.int32, (tok, tok), 1
    )
    counts = dot32(matched.astype(bf16), jnp.where(earlier, 1.0, 0.0).astype(bf16))
    rank = jnp.sum(matched * counts, axis=0, keepdims=True).astype(jnp.int32) - 1
    line = lax.broadcasted_iota(jnp.int32, (128, tok), 0)
    spread = jnp.where(line % capacity == rank, 1.0, 0.0).astype(bf16)
    both = (((1,), (1,)), ((), ()))
    codes = [
        lax.dot_general(
            (matched * part.astype(f32)).astype(bf16), spread, both, preferred_element_type=f32
        )
        for part in (slot // 128 + 1, slot % 128)
    ]
    first_half = lax.broadcasted_iota(jnp.int32, (shards, 128), 1) < capacity
    code = jnp.where(first_half, codes[0], codes[1])
    return code, owner * capacity + rank


def pack_kernel(*refs, capacity, rows_shard):
    sources, (out_ref, pos_ref), buffers, sems = refs[:7], refs[7:9], refs[9:16], refs[16]
    copies = [
        pltpu.make_async_copy(source, buffer, sems.at[i])
        for i, (source, buffer) in enumerate(zip(sources, buffers, strict=True))
    ]
    for copy in copies:
        copy.start()
    for copy in copies:
        copy.wait()
    cur_ref, prev_ref, grads_ref, places_ref, w_gate_ref, w_up_ref, w_out_ref = buffers
    shards = out_ref.shape[0]
    places = places_ref[...]
    parts = jnp.concatenate(
        [(places // 128).astype(f32), (places % 128).astype(f32)], axis=1
    ).astype(bf16)
    cur_code, cur_pos = packed(cur_ref[...], parts, capacity, shards, rows_shard)
    prev_code, prev_pos = packed(prev_ref[...], parts, capacity, shards, rows_shard)
    pos_ref[...] = cur_pos
    slots = shards * capacity
    slot_row = lax.broadcasted_iota(jnp.int32, (slots, prev_pos.shape[1]), 0)
    pack = jnp.where(slot_row == prev_pos, 1.0, 0.0).astype(bf16)
    rows = dot32(pack, grads_ref[...]).astype(bf16)
    at = lax.axis_index(XY)
    cut = (pl.ds(pl.multiple_of((at % 4) * 32, 32), 32), pl.ds(pl.multiple_of((at // 4) * 128, 128), 128))
    gate_slice = w_gate_ref[cut].astype(f32)
    up_slice = w_up_ref[cut].astype(f32)
    own = jnp.where(lax.axis_index("core") == 0, gate_slice, up_slice).astype(bf16)
    out = jnp.concatenate([w_out_ref[...].astype(f32), jnp.zeros((12, 128), f32)], axis=0)
    tail_row = lax.broadcasted_iota(jnp.int32, (16, 128), 0)
    for shard in range(shards):
        out_ref[shard, :capacity, :] = rows[shard * capacity : (shard + 1) * capacity]
        out_ref[shard, capacity : capacity + 32, :] = own
        tail = jnp.where(tail_row == 14, cur_code[shard : shard + 1], out)
        tail = jnp.where(tail_row == 15, prev_code[shard : shard + 1], tail)
        out_ref[shard, capacity + 32 : capacity + 48, :] = tail.astype(bf16)


def pack(cur_ids, prev_ids, prev_grads, row_place, w_gate, w_up, w_out, shards, capacity, rows_shard):
    vmem = pl.BlockSpec(memory_space=pltpu.VMEM)
    tok = cur_ids.shape[0]
    arrays = (
        cur_ids.reshape(1, tok), prev_ids.reshape(1, tok), prev_grads,
        row_place.reshape(-1, 128), w_gate, w_up, w_out.reshape(4, 128),
    )
    return pl.pallas_call(
        lambda *refs: pack_kernel(*refs, capacity=capacity, rows_shard=rows_shard),
        out_shape=(
            jax.ShapeDtypeStruct((shards, capacity + 48, 128), bf16),
            jax.ShapeDtypeStruct((1, tok), jnp.int32),
        ),
        in_specs=[pl.BlockSpec(memory_space=pltpu.HBM)] * len(arrays),
        out_specs=(vmem, vmem),
        scratch_shapes=[pltpu.VMEM(array.shape, array.dtype) for array in arrays]
        + [pltpu.SemaphoreType.DMA((len(arrays),))],
        compiler_params=pltpu.CompilerParams(vmem_limit_bytes=62 * 1024 * 1024),
        name="pack",
    )(*arrays)


def decoded(line, capacity):
    values = line.astype(jnp.int32)
    return ((values[..., :capacity] - 1) * 128 + values[..., capacity:]).reshape(-1)


def tower_kernel(
    answers_ref, target_ref, own_ref, other_ref, w_gate_ref, w_up_ref, shared_ref,
    gain_ref, labels_ref, emb_grad_ref, grads_ref, weights_s, gate_s, up_s, sig_s,
):
    tok = target_ref.shape[1]
    width = answers_ref.shape[1]
    shards, span = shared_ref.shape[:2]
    lines = own_ref.shape[0] // 16
    core = lax.axis_index("core")
    home = lax.axis_index("emb")
    weights_s[core] = own_ref[...]
    weights_s[1 - core] = other_ref[...]
    slot_row = lax.broadcasted_iota(jnp.int32, (answers_ref.shape[0], tok), 0)
    pick = jnp.where(target_ref[...] == slot_row, 1.0, 0.0).astype(bf16)
    values = lax.dot_general(
        pick, answers_ref[...], (((0,), (0,)), ((), ())), preferred_element_type=f32
    )
    turned = labels_ref[...].T
    column = lax.broadcasted_iota(jnp.int32, turned.shape, 1) == home
    targets = jnp.sum(jnp.where(column, turned, 0.0), axis=1, keepdims=True)
    inverse_rms = lax.rsqrt(jnp.mean(values * values, axis=1, keepdims=True) + norm_eps)
    gain = gain_ref[...]
    normed_wide = values * inverse_rms * gain
    normed = normed_wide.astype(bf16)
    normed_t = normed_wide.T.astype(bf16)

    def far_block(hop, half, side):
        tiles = []
        for tile in (2 * half, 2 * half + 1):
            quarters = [
                weights_s[side, pl.ds((tile * 4 + k) * lines + hop * 32, 32), :]
                for k in range(4)
            ]
            tiles.append(jnp.concatenate(quarters, axis=0))
        return jnp.concatenate(tiles, axis=1)

    def home_block(hop, half, side):
        return (w_gate_ref, w_up_ref)[side][:, half * 256 : (half + 1) * 256]

    def out_row(shard, half, j):
        return shared_ref[shard, pl.ds(span - 16 + 2 * half + j, 1), :].astype(f32)

    def forward(hop, total, block):
        shard = (home + 1 + hop) % shards
        for half in range(2):
            at = hop * 2 + half
            gate = dot32(normed, block(hop, half, 0))
            up = dot32(normed, block(hop, half, 1))
            sig = jax.nn.sigmoid(gate)
            gate_s[at] = gate
            up_s[at] = up
            sig_s[at] = sig
            hidden = (gate * sig * up).astype(bf16).astype(f32)
            for j in range(2):
                total = total + hidden[:, j * 128 : (j + 1) * 128] * out_row(shard, half, j)
        return total

    total = forward(shards - 1, jnp.zeros((tok, 128), f32), home_block)
    total = lax.fori_loop(0, shards - 1, lambda hop, t: forward(hop, t, far_block), total)
    logits = jnp.sum(total, axis=1, keepdims=True)
    slopes = loss_weight * (jax.nn.sigmoid(logits) - targets)

    across = (((1,), (1,)), ((), ()))

    def backward(hop, back, block):
        shard = (home + 1 + hop) % shards
        for half in range(2):
            at = hop * 2 + half
            gate = gate_s[at]
            up = up_s[at]
            sig = sig_s[at]
            out = jnp.concatenate([out_row(shard, half, j) for j in range(2)], axis=1)
            back_hidden = slopes * out
            back_gate = (back_hidden * up * sig * (1.0 + gate * (1.0 - sig))).astype(bf16)
            back_up = (back_hidden * (gate * sig)).astype(bf16)
            for side, part in ((0, back_gate), (1, back_up)):
                back = back + lax.dot_general(
                    part, block(hop, half, side), across, preferred_element_type=f32
                )
                grad = dot32(normed_t, part).astype(bf16)
                place = core if side == 0 else 1 - core
                for j in range(2):
                    tile = 2 * half + j
                    for k in range(4):
                        grads_ref[
                            place, pl.ds((tile * 4 + k) * shards * 32 + shard * 32, 32), :
                        ] = grad[k * 32 : (k + 1) * 32, j * 128 : (j + 1) * 128]
        return back

    back = backward(shards - 1, jnp.zeros((tok, width), f32), home_block)
    back = lax.fori_loop(0, shards - 1, lambda hop, b: backward(hop, b, far_block), back)
    scaled = back * gain
    emb_grad_ref[...] = inverse_rms * scaled - values * (
        inverse_rms * inverse_rms * inverse_rms
    ) * jnp.mean(values * scaled, axis=1, keepdims=True)


def tower(answers, target, own, other, w_gate, w_up, shared, gain, labels):
    tok = target.shape[1]
    width = answers.shape[1]
    shards = shared.shape[0]
    vmem = pl.BlockSpec(memory_space=pltpu.VMEM)
    return pl.pallas_call(
        tower_kernel,
        out_shape=(
            jax.ShapeDtypeStruct((tok, width), f32),
            jax.ShapeDtypeStruct((2, shards * 512, width), bf16),
        ),
        in_specs=[vmem] * 9,
        out_specs=(vmem, vmem),
        scratch_shapes=[pltpu.VMEM((2, *own.shape), bf16)]
        + [pltpu.VMEM((2 * shards, tok, 256), f32)] * 3,
        compiler_params=pltpu.CompilerParams(vmem_limit_bytes=24 * 1024 * 1024),
        cost_estimate=pl.CostEstimate(
            flops=6 * 2 * tok * width * 4096, bytes_accessed=5 << 20, transcendentals=2 << 20
        ),
        name="tower",
    )(
        answers, target, own, other, w_gate, w_up, shared,
        gain.reshape(1, -1), labels.reshape(shards, tok),
    )


def update_kernel(
    own_ref, other_ref, table_ref, accum_ref,
    new_table_ref, new_accum_ref, gate_ref, up_ref, both_s, *, scale,
):
    core = lax.axis_index("core")
    both_s[core] = own_ref[...]
    both_s[1 - core] = other_ref[...]
    plane, lines = own_ref.shape[:2]
    span = lines - 32
    for side, out_ref in ((0, gate_ref), (1, up_ref)):
        for q in range(plane):
            tile, k = q // 4, q % 4
            out_ref[k * 32 : (k + 1) * 32, tile * 128 : (tile + 1) * 128] = (
                both_s[side, q, :32, :].astype(f32) * scale
            )
            rows = pl.ds((2 * q + side) * span, span)
            grad = both_s[side, q, 32:, :].astype(f32)
            total = accum_ref[rows, :] + grad * grad
            new_accum_ref[rows, :] = total
            new_table_ref[rows, :] = table_ref[rows, :] - learn_rate * grad * lax.rsqrt(total)


def update(own, other, table, accum, scale):
    vmem = pl.BlockSpec(memory_space=pltpu.VMEM)
    part = jax.ShapeDtypeStruct((128, 512), f32)
    return pl.pallas_call(
        lambda *refs: update_kernel(*refs, scale=scale),
        out_shape=(
            jax.ShapeDtypeStruct(table.shape, f32),
            jax.ShapeDtypeStruct(table.shape, f32),
            part,
            part,
        ),
        in_specs=[vmem] * 4,
        out_specs=(vmem,) * 4,
        scratch_shapes=[pltpu.VMEM((2, *own.shape), bf16)],
        compiler_params=pltpu.CompilerParams(vmem_limit_bytes=12 * 1024 * 1024),
        name="update",
    )(own, other, table, accum)


def swapped(array, axis):
    return lax.ppermute(array, axis, [(0, 1), (1, 0)])


def step(
    cur_ids, prev_ids, prev_grads, row_place, table, accum, labels, gain, w_gate, w_up, w_out
):
    shards = lax.axis_size("emb")
    plane = lax.axis_size(XY)
    rows_shard, width = table.shape
    tok = cur_ids.shape[0]
    capacity = min(tok, 2 * tok // shards)
    slots = shards * capacity
    core = lax.axis_index("core")
    home = lax.axis_index("emb")
    payload, cur_pos = pack(
        cur_ids, prev_ids, prev_grads, row_place, w_gate, w_up, w_out,
        shards, capacity, rows_shard,
    )
    first = exchange(payload, "emb")
    got_rows = first[:, :capacity].reshape(slots, width)
    slices = first[:, capacity : capacity + 32]
    wanted = decoded(first[:, capacity + 46], capacity)
    got_slots = decoded(first[:, capacity + 47], capacity)

    row_ids = jnp.arange(rows_shard, dtype=jnp.int32)
    fetched = dot32(
        (wanted[:, None] == row_ids[None, :]).astype(bf16), table.astype(bf16)
    ).astype(bf16)
    answers = exchange(fetched.reshape(shards, capacity, width), "emb").reshape(slots, width)

    span = rows_shard // plane // 2
    half_ids = jnp.arange(rows_shard // 2, dtype=jnp.int32)
    half_ids = half_ids // span * (2 * span) + half_ids % span

    def half_sum(side):
        hot = (half_ids + side * span)[:, None] == got_slots[None, :]
        return dot32(hot.astype(bf16), got_rows).reshape(plane, span, width)

    pair_sent = swapped(half_sum(1 - core), "core")
    pair_own = half_sum(core)

    foreign = lax.dynamic_slice(
        jnp.concatenate([slices, slices], axis=0), (home + 1, 0, 0), (shards - 1, 32, 128)
    ).reshape((shards - 1) * 32, 128)
    own_weights = lax.all_gather(foreign, XY, axis=0, tiled=True)
    other_weights = swapped(own_weights, "core")
    answers, pair_own, pair_sent = lax.optimization_barrier((answers, pair_own, pair_sent))

    emb_grad, tower_grads = tower(
        answers, cur_pos, own_weights, other_weights, w_gate, w_up, first, gain, labels
    )

    received = swapped(tower_grads[1], "core")
    core_sum = (tower_grads[0].astype(f32) + received.astype(f32)).astype(bf16)
    pair_grad = (pair_own + pair_sent).astype(bf16)
    second = exchange(
        jnp.concatenate([core_sum.reshape(plane, shards * 32, 128), pair_grad], axis=1), XY
    )
    plane_sum = second[:, : shards * 32].astype(f32).sum(axis=0).astype(bf16)
    half_grad = second[:, shards * 32 :].astype(f32).sum(axis=0)
    total_grad = (half_grad + swapped(half_grad, "zh")).astype(bf16)
    for_z = jnp.broadcast_to(plane_sum.reshape(1, shards, 32, 128), (2, shards, 32, 128))
    third = exchange(for_z.reshape(2 * shards, 32, 128), ZZ)
    tower_sum = third.astype(f32).sum(axis=0).astype(bf16)
    own = to_all(jnp.concatenate([tower_sum, total_grad], axis=0), XY)
    other = swapped(own, "core")

    tower_scale = 1.0 / math.sqrt(tok * shards * lax.axis_size(DP))
    new_table, new_accum, gate_sum, up_sum = update(own, other, table, accum, tower_scale)
    return (new_table, new_accum, gate_sum, up_sum, emb_grad)


def solution(mesh):
    torus = Mesh(mesh.devices.reshape(4, 4, 2, 2, mesh.shape["emb"]), DP_EMB)
    return jax.shard_map(
        step,
        mesh=torus,
        in_specs=(
            P(DP_EMB),
            P(DP_EMB),
            P(DP_EMB, None),
            P(),
            P("emb", None),
            P("emb", None),
            P(DP),
            P(),
            P(None, "emb"),
            P(None, "emb"),
            P("emb"),
        ),
        out_specs=(P("emb", None), P("emb", None), P(None, "emb"), P(None, "emb"), P(DP_EMB, None)),
        check_vma=False,
    )
```

```python
import math

import jax
import jax.numpy as jnp
from jax import lax
from jax.experimental import pallas as pl
from jax.experimental.pallas import tpu as pltpu
from jax.sharding import Mesh
from jax.sharding import PartitionSpec as P


DP = ("x", "y", "zh", "core")
DP_EMB = ("x", "y", "zh", "core", "emb")
XY = ("x", "y")
ZZ = ("zh", "emb")

loss_weight = 64.0
learn_rate = 0.1
norm_eps = 1e-06

bf16 = jnp.bfloat16
f32 = jnp.float32


def exchange(pieces, axis):
    return lax.all_to_all(pieces, axis, 0, 0, tiled=True)


def to_all(array, axis):
    return exchange(jnp.broadcast_to(array[None], (lax.axis_size(axis), *array.shape)), axis)


def dot32(a, b):
    return jnp.dot(a, b, preferred_element_type=f32)


def packed(ids, parts, capacity, shards, rows_shard):
    tok = ids.shape[1]
    lines = parts.shape[0]
    row = lax.broadcasted_iota(jnp.int32, (lines, tok), 0)
    pick = jnp.where(ids // 128 == row, 1.0, 0.0).astype(bf16)
    found = lax.dot_general(parts, pick, (((0,), (0,)), ((), ())), preferred_element_type=f32)
    lane = lax.broadcasted_iota(jnp.int32, (128, tok), 0) == ids % 128
    high = jnp.sum(jnp.where(lane, found[:128], 0.0), axis=0, keepdims=True)
    low = jnp.sum(jnp.where(lane, found[128:], 0.0), axis=0, keepdims=True)
    place = (high * 128.0 + low).astype(jnp.int32)
    shard = lax.broadcasted_iota(jnp.int32, (shards, tok), 0)
    match = (place >= shard * rows_shard) & (place < (shard + 1) * rows_shard)
    matched = jnp.where(match, 1.0, 0.0)
    owner = jnp.sum(jnp.where(match, shard, 0), axis=0, keepdims=True)
    slot = place - owner * rows_shard
    earlier = lax.broadcasted_iota(jnp.int32, (tok, tok), 0) <= lax.broadcasted_iota(
        jnp.int32, (tok, tok), 1
    )
    counts = dot32(matched.astype(bf16), jnp.where(earlier, 1.0, 0.0).astype(bf16))
    rank = jnp.sum(matched * counts, axis=0, keepdims=True).astype(jnp.int32) - 1
    line = lax.broadcasted_iota(jnp.int32, (128, tok), 0)
    spread = jnp.where(line % capacity == rank, 1.0, 0.0).astype(bf16)
    both = (((1,), (1,)), ((), ()))
    codes = [
        lax.dot_general(
            (matched * part.astype(f32)).astype(bf16), spread, both, preferred_element_type=f32
        )
        for part in (slot // 128 + 1, slot % 128)
    ]
    first_half = lax.broadcasted_iota(jnp.int32, (shards, 128), 1) < capacity
    code = jnp.where(first_half, codes[0], codes[1])
    return code, owner * capacity + rank


def pack_kernel(*refs, capacity, rows_shard):
    sources, (out_ref, pos_ref), buffers, sems = refs[:7], refs[7:9], refs[9:16], refs[16]
    copies = [
        pltpu.make_async_copy(source, buffer, sems.at[i])
        for i, (source, buffer) in enumerate(zip(sources, buffers, strict=True))
    ]
    for i in (0, 1, 3, 2, 4, 5, 6):
        copies[i].start()
    for i in (0, 1, 3):
        copies[i].wait()
    cur_ref, prev_ref, grads_ref, places_ref, w_gate_ref, w_up_ref, w_out_ref = buffers
    shards = out_ref.shape[0]
    places = places_ref[...]
    parts = jnp.concatenate(
        [(places // 128).astype(f32), (places % 128).astype(f32)], axis=1
    ).astype(bf16)
    cur_code, cur_pos = packed(cur_ref[...], parts, capacity, shards, rows_shard)
    prev_code, prev_pos = packed(prev_ref[...], parts, capacity, shards, rows_shard)
    pos_ref[...] = cur_pos
    slots = shards * capacity
    slot_row = lax.broadcasted_iota(jnp.int32, (slots, prev_pos.shape[1]), 0)
    pack = jnp.where(slot_row == prev_pos, 1.0, 0.0).astype(bf16)
    for i in (2, 4, 5, 6):
        copies[i].wait()
    rows = dot32(pack, grads_ref[...]).astype(bf16)
    at = lax.axis_index(XY)
    cut = (pl.ds(pl.multiple_of((at % 4) * 32, 32), 32), pl.ds(pl.multiple_of((at // 4) * 128, 128), 128))
    gate_slice = w_gate_ref[cut].astype(f32)
    up_slice = w_up_ref[cut].astype(f32)
    own = jnp.where(lax.axis_index("core") == 0, gate_slice, up_slice).astype(bf16)
    out = jnp.concatenate([w_out_ref[...].astype(f32), jnp.zeros((12, 128), f32)], axis=0)
    tail_row = lax.broadcasted_iota(jnp.int32, (16, 128), 0)
    for shard in range(shards):
        out_ref[shard, :capacity, :] = rows[shard * capacity : (shard + 1) * capacity]
        out_ref[shard, capacity : capacity + 32, :] = own
        tail = jnp.where(tail_row == 14, cur_code[shard : shard + 1], out)
        tail = jnp.where(tail_row == 15, prev_code[shard : shard + 1], tail)
        out_ref[shard, capacity + 32 : capacity + 48, :] = tail.astype(bf16)


def pack(cur_ids, prev_ids, prev_grads, row_place, w_gate, w_up, w_out, shards, capacity, rows_shard):
    vmem = pl.BlockSpec(memory_space=pltpu.VMEM)
    tok = cur_ids.shape[0]
    arrays = (
        cur_ids.reshape(1, tok), prev_ids.reshape(1, tok), prev_grads,
        row_place.reshape(-1, 128), w_gate, w_up, w_out.reshape(4, 128),
    )
    return pl.pallas_call(
        lambda *refs: pack_kernel(*refs, capacity=capacity, rows_shard=rows_shard),
        out_shape=(
            jax.ShapeDtypeStruct((shards, capacity + 48, 128), bf16),
            jax.ShapeDtypeStruct((1, tok), jnp.int32),
        ),
        in_specs=[pl.BlockSpec(memory_space=pltpu.HBM)] * len(arrays),
        out_specs=(vmem, vmem),
        scratch_shapes=[pltpu.VMEM(array.shape, array.dtype) for array in arrays]
        + [pltpu.SemaphoreType.DMA((len(arrays),))],
        compiler_params=pltpu.CompilerParams(vmem_limit_bytes=62 * 1024 * 1024),
        name="pack",
    )(*arrays)


def decoded(line, capacity):
    values = line.astype(jnp.int32)
    return ((values[..., :capacity] - 1) * 128 + values[..., capacity:]).reshape(-1)


def tower_kernel(
    answers_ref, target_ref, own_ref, other_ref, w_gate_ref, w_up_ref, shared_ref,
    gain_ref, labels_ref, table_part_ref, emb_grad_ref, grads_ref, weights_s, gate_s, up_s,
):
    tok = target_ref.shape[1]
    width = answers_ref.shape[1]
    shards, span = shared_ref.shape[:2]
    lines = own_ref.shape[0] // 16
    core = lax.axis_index("core")
    home = lax.axis_index("emb")
    weights_s[core] = own_ref[...]
    weights_s[1 - core] = other_ref[...]
    slot_row = lax.broadcasted_iota(jnp.int32, (answers_ref.shape[0], tok), 0)
    pick = jnp.where(target_ref[...] == slot_row, 1.0, 0.0).astype(bf16)
    values = lax.dot_general(
        pick, answers_ref[...], (((0,), (0,)), ((), ())), preferred_element_type=f32
    )
    turned = labels_ref[...].T
    column = lax.broadcasted_iota(jnp.int32, turned.shape, 1) == home
    targets = jnp.sum(jnp.where(column, turned, 0.0), axis=1, keepdims=True)
    inverse_rms = lax.rsqrt(jnp.mean(values * values, axis=1, keepdims=True) + norm_eps)
    gain = gain_ref[...]
    normed_wide = values * inverse_rms * gain
    normed = normed_wide.astype(bf16)
    normed_t = normed_wide.T.astype(bf16)

    def far_block(hop, half, side):
        tiles = []
        for tile in (2 * half, 2 * half + 1):
            quarters = [
                weights_s[side, pl.ds((tile * 4 + k) * lines + hop * 32, 32), :]
                for k in range(4)
            ]
            tiles.append(jnp.concatenate(quarters, axis=0))
        return jnp.concatenate(tiles, axis=1)

    def home_block(hop, half, side):
        return (w_gate_ref, w_up_ref)[side][:, half * 256 : (half + 1) * 256]

    def out_row(shard, half, j):
        return shared_ref[shard, pl.ds(span - 16 + 2 * half + j, 1), :].astype(f32)

    def forward(hop, total, block):
        shard = (home + 1 + hop) % shards
        for half in range(2):
            at = hop * 2 + half
            gate = dot32(normed, block(hop, half, 0))
            up = dot32(normed, block(hop, half, 1))
            sig = jax.nn.sigmoid(gate)
            act = gate * sig
            gate_s[at] = up * (sig + act * (1.0 - sig))
            up_s[at] = act
            hidden = (act * up).astype(bf16).astype(f32)
            for j in range(2):
                total = total + hidden[:, j * 128 : (j + 1) * 128] * out_row(shard, half, j)
        return total

    total = forward(shards - 1, jnp.zeros((tok, 128), f32), home_block)
    total = lax.fori_loop(0, shards - 1, lambda hop, t: forward(hop, t, far_block), total)
    logits = jnp.sum(total, axis=1, keepdims=True)
    slopes = loss_weight * (jax.nn.sigmoid(logits) - targets)

    across = (((1,), (1,)), ((), ()))

    def backward(hop, back, block):
        shard = (home + 1 + hop) % shards
        for half in range(2):
            at = hop * 2 + half
            out = jnp.concatenate([out_row(shard, half, j) for j in range(2)], axis=1)
            back_hidden = slopes * out
            back_gate = (back_hidden * gate_s[at]).astype(bf16)
            back_up = (back_hidden * up_s[at]).astype(bf16)
            for side, part in ((0, back_gate), (1, back_up)):
                back = back + lax.dot_general(
                    part, block(hop, half, side), across, preferred_element_type=f32
                )
                grad = dot32(normed_t, part).astype(bf16)
                place = core if side == 0 else 1 - core
                for j in range(2):
                    tile = 2 * half + j
                    for k in range(4):
                        grads_ref[
                            place, tile * 4 + k, pl.ds(shard * 32, 32), :
                        ] = grad[k * 32 : (k + 1) * 32, j * 128 : (j + 1) * 128]
        return back

    back = backward(shards - 1, jnp.zeros((tok, width), f32), home_block)
    back = lax.fori_loop(0, shards - 1, lambda hop, b: backward(hop, b, far_block), back)
    grads_ref[:, :, shards * 32 :, :] = table_part_ref[...].astype(bf16)
    scaled = back * gain
    emb_grad_ref[...] = inverse_rms * scaled - values * (
        inverse_rms * inverse_rms * inverse_rms
    ) * jnp.mean(values * scaled, axis=1, keepdims=True)


def tower(answers, target, own, other, w_gate, w_up, shared, gain, labels, table_part):
    tok = target.shape[1]
    width = answers.shape[1]
    shards = shared.shape[0]
    vmem = pl.BlockSpec(memory_space=pltpu.VMEM)
    return pl.pallas_call(
        tower_kernel,
        out_shape=(
            jax.ShapeDtypeStruct((tok, width), f32),
            jax.ShapeDtypeStruct((2, 16, shards * 32 + table_part.shape[2], width), bf16),
        ),
        in_specs=[vmem] * 10,
        out_specs=(vmem, vmem),
        scratch_shapes=[pltpu.VMEM((2, *own.shape), bf16)]
        + [pltpu.VMEM((2 * shards, tok, 256), f32)] * 2,
        compiler_params=pltpu.CompilerParams(vmem_limit_bytes=20 * 1024 * 1024),
        cost_estimate=pl.CostEstimate(
            flops=6 * 2 * tok * width * 4096, bytes_accessed=5 << 20, transcendentals=2 << 20
        ),
        name="tower",
    )(
        answers, target, own, other, w_gate, w_up, shared,
        gain.reshape(1, -1), labels.reshape(shards, tok), table_part,
    )


def update_kernel(
    own_ref, other_ref, table_ref, accum_ref,
    new_table_ref, new_accum_ref, gate_ref, up_ref, both_s, *, scale,
):
    core = lax.axis_index("core")
    both_s[core] = own_ref[...]
    both_s[1 - core] = other_ref[...]
    plane, lines = own_ref.shape[:2]
    span = lines - 32
    for side, out_ref in ((0, gate_ref), (1, up_ref)):
        for q in range(plane):
            tile, k = q // 4, q % 4
            out_ref[k * 32 : (k + 1) * 32, tile * 128 : (tile + 1) * 128] = (
                both_s[side, q, :32, :].astype(f32) * scale
            )
            rows = pl.ds((2 * q + side) * span, span)
            grad = both_s[side, q, 32:, :].astype(f32)
            total = accum_ref[rows, :] + grad * grad
            new_accum_ref[rows, :] = total
            new_table_ref[rows, :] = table_ref[rows, :] - learn_rate * grad * lax.rsqrt(total)


def update(own, other, table, accum, scale):
    vmem = pl.BlockSpec(memory_space=pltpu.VMEM)
    part = jax.ShapeDtypeStruct((128, 512), f32)
    return pl.pallas_call(
        lambda *refs: update_kernel(*refs, scale=scale),
        out_shape=(
            jax.ShapeDtypeStruct(table.shape, f32),
            jax.ShapeDtypeStruct(table.shape, f32),
            part,
            part,
        ),
        in_specs=[vmem] * 4,
        out_specs=(vmem,) * 4,
        scratch_shapes=[pltpu.VMEM((2, *own.shape), bf16)],
        compiler_params=pltpu.CompilerParams(vmem_limit_bytes=12 * 1024 * 1024),
        name="update",
    )(own, other, table, accum)


def swapped(array, axis):
    return lax.ppermute(array, axis, [(0, 1), (1, 0)])


def step(
    cur_ids, prev_ids, prev_grads, row_place, table, accum, labels, gain, w_gate, w_up, w_out
):
    shards = lax.axis_size("emb")
    plane = lax.axis_size(XY)
    rows_shard, width = table.shape
    tok = cur_ids.shape[0]
    capacity = min(tok, 2 * tok // shards)
    slots = shards * capacity
    core = lax.axis_index("core")
    home = lax.axis_index("emb")
    payload, cur_pos = pack(
        cur_ids, prev_ids, prev_grads, row_place, w_gate, w_up, w_out,
        shards, capacity, rows_shard,
    )
    first = exchange(payload, "emb")
    rows_table = lax.optimization_barrier(table.astype(bf16))
    got_rows = first[:, :capacity].reshape(slots, width)
    slices = first[:, capacity : capacity + 32]
    wanted = decoded(first[:, capacity + 46], capacity)
    got_slots = decoded(first[:, capacity + 47], capacity)

    row_ids = jnp.arange(rows_shard, dtype=jnp.int32)
    fetched = dot32(
        (wanted[:, None] == row_ids[None, :]).astype(bf16), rows_table
    ).astype(bf16)
    answers = exchange(fetched.reshape(shards, capacity, width), "emb").reshape(slots, width)

    span = rows_shard // plane // 2
    half_ids = jnp.arange(rows_shard // 2, dtype=jnp.int32)
    half_ids = half_ids // span * (2 * span) + half_ids % span
    part_ids = jnp.concatenate([half_ids + core * span, half_ids + (1 - core) * span])
    table_part = dot32((part_ids[:, None] == got_slots[None, :]).astype(bf16), got_rows)
    table_part = table_part.reshape(2, plane, span, width)

    foreign = lax.dynamic_slice(
        jnp.concatenate([slices, slices], axis=0), (home + 1, 0, 0), (shards - 1, 32, 128)
    ).reshape((shards - 1) * 32, 128)
    own_weights = lax.all_gather(foreign, XY, axis=0, tiled=True)
    other_weights = swapped(own_weights, "core")
    emb_grad, tower_grads = tower(
        answers, cur_pos, own_weights, other_weights, w_gate, w_up, first, gain, labels,
        table_part,
    )

    received = swapped(tower_grads[1], "core")
    core_sum = (tower_grads[0].astype(f32) + received.astype(f32)).astype(bf16)
    second = exchange(core_sum, XY)
    plane_sum = second[:, : shards * 32].astype(f32).sum(axis=0).astype(bf16)
    half_grad = second[:, shards * 32 :].astype(f32).sum(axis=0)
    total_grad = (half_grad + swapped(half_grad, "zh")).astype(bf16)
    for_z = jnp.broadcast_to(plane_sum.reshape(1, shards, 32, 128), (2, shards, 32, 128))
    third = exchange(for_z.reshape(2 * shards, 32, 128), ZZ)
    tower_sum = third.astype(f32).sum(axis=0).astype(bf16)
    own = to_all(jnp.concatenate([tower_sum, total_grad], axis=0), XY)
    other = swapped(own, "core")

    tower_scale = 1.0 / math.sqrt(tok * shards * lax.axis_size(DP))
    new_table, new_accum, gate_sum, up_sum = update(own, other, table, accum, tower_scale)
    return (new_table, new_accum, gate_sum, up_sum, emb_grad)


def solution(mesh):
    torus = Mesh(mesh.devices.reshape(4, 4, 2, 2, mesh.shape["emb"]), DP_EMB)
    return jax.shard_map(
        step,
        mesh=torus,
        in_specs=(
            P(DP_EMB),
            P(DP_EMB),
            P(DP_EMB, None),
            P(),
            P("emb", None),
            P("emb", None),
            P(DP),
            P(),
            P(None, "emb"),
            P(None, "emb"),
            P("emb"),
        ),
        out_specs=(P("emb", None), P("emb", None), P(None, "emb"), P(None, "emb"), P(DP_EMB, None)),
        check_vma=False,
    )
```

```python
import math

import jax
import jax.numpy as jnp
from jax import lax
from jax.experimental import pallas as pl
from jax.experimental.pallas import tpu as pltpu
from jax.sharding import Mesh
from jax.sharding import PartitionSpec as P


DP = ("x", "y", "zh", "core")
DP_EMB = ("x", "y", "zh", "core", "emb")
XY = ("x", "y")
ZZ = ("zh", "emb")

loss_weight = 64.0
learn_rate = 0.1
norm_eps = 1e-06

bf16 = jnp.bfloat16
f32 = jnp.float32


def exchange(pieces, axis):
    return lax.all_to_all(pieces, axis, 0, 0, tiled=True)


def to_all(array, axis):
    return exchange(jnp.broadcast_to(array[None], (lax.axis_size(axis), *array.shape)), axis)


def dot32(a, b):
    return jnp.dot(a, b, preferred_element_type=f32)


def packed(ids, parts, capacity, shards, rows_shard):
    tok = ids.shape[1]
    lines = parts.shape[0]
    row = lax.broadcasted_iota(jnp.int32, (lines, tok), 0)
    pick = jnp.where(ids // 128 == row, 1.0, 0.0).astype(bf16)
    found = lax.dot_general(parts, pick, (((0,), (0,)), ((), ())), preferred_element_type=f32)
    lane = lax.broadcasted_iota(jnp.int32, (128, tok), 0) == ids % 128
    high = jnp.sum(jnp.where(lane, found[:128], 0.0), axis=0, keepdims=True)
    low = jnp.sum(jnp.where(lane, found[128:], 0.0), axis=0, keepdims=True)
    place = (high * 128.0 + low).astype(jnp.int32)
    shard = lax.broadcasted_iota(jnp.int32, (shards, tok), 0)
    match = (place >= shard * rows_shard) & (place < (shard + 1) * rows_shard)
    matched = jnp.where(match, 1.0, 0.0)
    owner = jnp.sum(jnp.where(match, shard, 0), axis=0, keepdims=True)
    slot = place - owner * rows_shard
    earlier = lax.broadcasted_iota(jnp.int32, (tok, tok), 0) <= lax.broadcasted_iota(
        jnp.int32, (tok, tok), 1
    )
    counts = dot32(matched.astype(bf16), jnp.where(earlier, 1.0, 0.0).astype(bf16))
    rank = jnp.sum(matched * counts, axis=0, keepdims=True).astype(jnp.int32) - 1
    line = lax.broadcasted_iota(jnp.int32, (128, tok), 0)
    spread = jnp.where(line % capacity == rank, 1.0, 0.0).astype(bf16)
    both = (((1,), (1,)), ((), ()))
    codes = [
        lax.dot_general(
            (matched * part.astype(f32)).astype(bf16), spread, both, preferred_element_type=f32
        )
        for part in (slot // 128 + 1, slot % 128)
    ]
    first_half = lax.broadcasted_iota(jnp.int32, (shards, 128), 1) < capacity
    code = jnp.where(first_half, codes[0], codes[1])
    return code, owner * capacity + rank


def pack_kernel(*refs, capacity, rows_shard):
    sources, (out_ref, pos_ref), buffers, sems = refs[:7], refs[7:9], refs[9:16], refs[16]
    copies = [
        pltpu.make_async_copy(source, buffer, sems.at[i])
        for i, (source, buffer) in enumerate(zip(sources, buffers, strict=True))
    ]
    for i in (0, 1, 3, 2, 4, 5, 6):
        copies[i].start()
    for i in (0, 1, 3):
        copies[i].wait()
    cur_ref, prev_ref, grads_ref, places_ref, w_gate_ref, w_up_ref, w_out_ref = buffers
    shards = out_ref.shape[0]
    places = places_ref[...]
    parts = jnp.concatenate(
        [(places // 128).astype(f32), (places % 128).astype(f32)], axis=1
    ).astype(bf16)
    cur_code, cur_pos = packed(cur_ref[...], parts, capacity, shards, rows_shard)
    prev_code, prev_pos = packed(prev_ref[...], parts, capacity, shards, rows_shard)
    pos_ref[...] = cur_pos
    slots = shards * capacity
    slot_row = lax.broadcasted_iota(jnp.int32, (slots, prev_pos.shape[1]), 0)
    pack = jnp.where(slot_row == prev_pos, 1.0, 0.0).astype(bf16)
    for i in (2, 4, 5, 6):
        copies[i].wait()
    rows = dot32(pack, grads_ref[...]).astype(bf16)
    at = lax.axis_index(XY)
    cut = (pl.ds(pl.multiple_of((at % 4) * 32, 32), 32), pl.ds(pl.multiple_of((at // 4) * 128, 128), 128))
    gate_slice = w_gate_ref[cut].astype(f32)
    up_slice = w_up_ref[cut].astype(f32)
    own = jnp.where(lax.axis_index("core") == 0, gate_slice, up_slice).astype(bf16)
    out = jnp.concatenate([w_out_ref[...].astype(f32), jnp.zeros((12, 128), f32)], axis=0)
    tail_row = lax.broadcasted_iota(jnp.int32, (16, 128), 0)
    for shard in range(shards):
        out_ref[shard, :capacity, :] = rows[shard * capacity : (shard + 1) * capacity]
        out_ref[shard, capacity : capacity + 32, :] = own
        tail = jnp.where(tail_row == 14, cur_code[shard : shard + 1], out)
        tail = jnp.where(tail_row == 15, prev_code[shard : shard + 1], tail)
        out_ref[shard, capacity + 32 : capacity + 48, :] = tail.astype(bf16)


def pack(cur_ids, prev_ids, prev_grads, row_place, w_gate, w_up, w_out, shards, capacity, rows_shard):
    vmem = pl.BlockSpec(memory_space=pltpu.VMEM)
    tok = cur_ids.shape[0]
    arrays = (
        cur_ids.reshape(1, tok), prev_ids.reshape(1, tok), prev_grads,
        row_place.reshape(-1, 128), w_gate, w_up, w_out.reshape(4, 128),
    )
    return pl.pallas_call(
        lambda *refs: pack_kernel(*refs, capacity=capacity, rows_shard=rows_shard),
        out_shape=(
            jax.ShapeDtypeStruct((shards, capacity + 48, 128), bf16),
            jax.ShapeDtypeStruct((1, tok), jnp.int32),
        ),
        in_specs=[pl.BlockSpec(memory_space=pltpu.HBM)] * len(arrays),
        out_specs=(vmem, vmem),
        scratch_shapes=[pltpu.VMEM(array.shape, array.dtype) for array in arrays]
        + [pltpu.SemaphoreType.DMA((len(arrays),))],
        compiler_params=pltpu.CompilerParams(vmem_limit_bytes=62 * 1024 * 1024),
        name="pack",
    )(*arrays)


def decoded(line, capacity):
    values = line.astype(jnp.int32)
    return ((values[..., :capacity] - 1) * 128 + values[..., capacity:]).reshape(-1)


def tower_kernel(
    answers_ref, target_ref, own_ref, other_ref, w_gate_ref, w_up_ref, shared_ref,
    gain_ref, labels_ref, table_part_ref, emb_grad_ref, grads_ref, weights_s, gate_s, up_s,
):
    tok = target_ref.shape[1]
    width = answers_ref.shape[1]
    shards, span = shared_ref.shape[:2]
    lines = own_ref.shape[0] // 16
    core = lax.axis_index("core")
    home = lax.axis_index("emb")
    weights_s[core] = own_ref[...]
    weights_s[1 - core] = other_ref[...]
    slot_row = lax.broadcasted_iota(jnp.int32, (answers_ref.shape[0], tok), 0)
    pick = jnp.where(target_ref[...] == slot_row, 1.0, 0.0).astype(bf16)
    values = lax.dot_general(
        pick, answers_ref[...], (((0,), (0,)), ((), ())), preferred_element_type=f32
    )
    turned = labels_ref[...].T
    column = lax.broadcasted_iota(jnp.int32, turned.shape, 1) == home
    targets = jnp.sum(jnp.where(column, turned, 0.0), axis=1, keepdims=True)
    inverse_rms = lax.rsqrt(jnp.mean(values * values, axis=1, keepdims=True) + norm_eps)
    gain = gain_ref[...]
    normed_wide = values * inverse_rms * gain
    normed = normed_wide.astype(bf16)
    normed_t = normed_wide.T.astype(bf16)

    def far_block(hop, half, side):
        tiles = []
        for tile in (2 * half, 2 * half + 1):
            quarters = [
                weights_s[side, pl.ds((tile * 4 + k) * lines + hop * 32, 32), :]
                for k in range(4)
            ]
            tiles.append(jnp.concatenate(quarters, axis=0))
        return jnp.concatenate(tiles, axis=1)

    def home_block(hop, half, side):
        return (w_gate_ref, w_up_ref)[side][:, half * 256 : (half + 1) * 256]

    def out_row(shard, half, j):
        return shared_ref[shard, pl.ds(span - 16 + 2 * half + j, 1), :].astype(f32)

    def forward(hop, total, block):
        shard = (home + 1 + hop) % shards
        for half in range(2):
            at = hop * 2 + half
            gate = dot32(normed, block(hop, half, 0))
            up = dot32(normed, block(hop, half, 1))
            sig = jax.nn.sigmoid(gate)
            act = gate * sig
            gate_s[at] = up * (sig + act * (1.0 - sig))
            up_s[at] = act
            hidden = (act * up).astype(bf16).astype(f32)
            for j in range(2):
                total = total + hidden[:, j * 128 : (j + 1) * 128] * out_row(shard, half, j)
        return total

    total = forward(shards - 1, jnp.zeros((tok, 128), f32), home_block)
    total = lax.fori_loop(0, shards - 1, lambda hop, t: forward(hop, t, far_block), total, unroll=True)
    logits = jnp.sum(total, axis=1, keepdims=True)
    slopes = loss_weight * (jax.nn.sigmoid(logits) - targets)

    across = (((1,), (1,)), ((), ()))

    def backward(hop, back, block):
        shard = (home + 1 + hop) % shards
        for half in range(2):
            at = hop * 2 + half
            out = jnp.concatenate([out_row(shard, half, j) for j in range(2)], axis=1)
            back_hidden = slopes * out
            back_gate = (back_hidden * gate_s[at]).astype(bf16)
            back_up = (back_hidden * up_s[at]).astype(bf16)
            for side, part in ((0, back_gate), (1, back_up)):
                back = back + lax.dot_general(
                    part, block(hop, half, side), across, preferred_element_type=f32
                )
                grad = dot32(normed_t, part).astype(bf16)
                place = core if side == 0 else 1 - core
                for j in range(2):
                    tile = 2 * half + j
                    for k in range(4):
                        grads_ref[
                            place, tile * 4 + k, pl.ds(shard * 32, 32), :
                        ] = grad[k * 32 : (k + 1) * 32, j * 128 : (j + 1) * 128]
        return back

    back = backward(shards - 1, jnp.zeros((tok, width), f32), home_block)
    back = lax.fori_loop(0, shards - 1, lambda hop, b: backward(hop, b, far_block), back, unroll=True)
    grads_ref[:, :, shards * 32 :, :] = table_part_ref[...]
    scaled = back * gain
    emb_grad_ref[...] = inverse_rms * scaled - values * (
        inverse_rms * inverse_rms * inverse_rms
    ) * jnp.mean(values * scaled, axis=1, keepdims=True)


def tower(answers, target, own, other, w_gate, w_up, shared, gain, labels, table_part):
    tok = target.shape[1]
    width = answers.shape[1]
    shards = shared.shape[0]
    vmem = pl.BlockSpec(memory_space=pltpu.VMEM)
    return pl.pallas_call(
        tower_kernel,
        out_shape=(
            jax.ShapeDtypeStruct((tok, width), f32),
            jax.ShapeDtypeStruct((2, 16, shards * 32 + table_part.shape[2], width), bf16),
        ),
        in_specs=[vmem] * 10,
        out_specs=(vmem, vmem),
        scratch_shapes=[pltpu.VMEM((2, *own.shape), bf16)]
        + [pltpu.VMEM((2 * shards, tok, 256), f32)] * 2,
        compiler_params=pltpu.CompilerParams(vmem_limit_bytes=20 * 1024 * 1024),
        cost_estimate=pl.CostEstimate(
            flops=6 * 2 * tok * width * 4096, bytes_accessed=5 << 20, transcendentals=2 << 20
        ),
        name="tower",
    )(
        answers, target, own, other, w_gate, w_up, shared,
        gain.reshape(1, -1), labels.reshape(shards, tok), table_part,
    )


def update_kernel(
    own_ref, other_ref, table_ref, accum_ref,
    new_table_ref, new_accum_ref, gate_ref, up_ref, both_s, *, scale,
):
    core = lax.axis_index("core")
    both_s[core] = own_ref[...]
    both_s[1 - core] = other_ref[...]
    plane, lines = own_ref.shape[:2]
    span = lines - 32
    for side, out_ref in ((0, gate_ref), (1, up_ref)):
        for q in range(plane):
            tile, k = q // 4, q % 4
            out_ref[k * 32 : (k + 1) * 32, tile * 128 : (tile + 1) * 128] = (
                both_s[side, q, :32, :].astype(f32) * scale
            )
            rows = pl.ds((2 * q + side) * span, span)
            grad = both_s[side, q, 32:, :].astype(f32)
            total = accum_ref[rows, :] + grad * grad
            new_accum_ref[rows, :] = total
            new_table_ref[rows, :] = table_ref[rows, :] - learn_rate * grad * lax.rsqrt(total)


def update(own, other, table, accum, scale):
    vmem = pl.BlockSpec(memory_space=pltpu.VMEM)
    part = jax.ShapeDtypeStruct((128, 512), f32)
    return pl.pallas_call(
        lambda *refs: update_kernel(*refs, scale=scale),
        out_shape=(
            jax.ShapeDtypeStruct(table.shape, f32),
            jax.ShapeDtypeStruct(table.shape, f32),
            part,
            part,
        ),
        in_specs=[vmem] * 4,
        out_specs=(vmem,) * 4,
        scratch_shapes=[pltpu.VMEM((2, *own.shape), bf16)],
        compiler_params=pltpu.CompilerParams(vmem_limit_bytes=12 * 1024 * 1024),
        name="update",
    )(own, other, table, accum)


def swapped(array, axis):
    return lax.ppermute(array, axis, [(0, 1), (1, 0)])


def step(
    cur_ids, prev_ids, prev_grads, row_place, table, accum, labels, gain, w_gate, w_up, w_out
):
    shards = lax.axis_size("emb")
    plane = lax.axis_size(XY)
    rows_shard, width = table.shape
    tok = cur_ids.shape[0]
    capacity = min(tok, 2 * tok // shards)
    slots = shards * capacity
    core = lax.axis_index("core")
    home = lax.axis_index("emb")
    payload, cur_pos = pack(
        cur_ids, prev_ids, prev_grads, row_place, w_gate, w_up, w_out,
        shards, capacity, rows_shard,
    )
    first = exchange(payload, "emb")
    rows_table = lax.optimization_barrier(table.astype(bf16))
    got_rows = first[:, :capacity].reshape(slots, width)
    slices = first[:, capacity : capacity + 32]
    wanted = decoded(first[:, capacity + 46], capacity)
    got_slots = decoded(first[:, capacity + 47], capacity)

    row_ids = jnp.arange(rows_shard, dtype=jnp.int32)
    fetched = dot32(
        (wanted[:, None] == row_ids[None, :]).astype(bf16), rows_table
    ).astype(bf16)
    answers = exchange(fetched.reshape(shards, capacity, width), "emb").reshape(slots, width)

    span = rows_shard // plane // 2
    half_ids = jnp.arange(rows_shard // 2, dtype=jnp.int32)
    half_ids = half_ids // span * (2 * span) + half_ids % span
    part_ids = jnp.concatenate([half_ids + core * span, half_ids + (1 - core) * span])
    table_part = dot32((part_ids[:, None] == got_slots[None, :]).astype(bf16), got_rows)
    table_part = table_part.astype(bf16).reshape(2, plane, span, width)

    foreign = lax.dynamic_slice(
        jnp.concatenate([slices, slices], axis=0), (home + 1, 0, 0), (shards - 1, 32, 128)
    ).reshape((shards - 1) * 32, 128)
    own_weights = lax.all_gather(foreign, XY, axis=0, tiled=True)
    other_weights = swapped(own_weights, "core")
    emb_grad, tower_grads = tower(
        answers, cur_pos, own_weights, other_weights, w_gate, w_up, first, gain, labels,
        table_part,
    )

    received = swapped(tower_grads[1], "core")
    core_sum = (tower_grads[0].astype(f32) + received.astype(f32)).astype(bf16)
    second = exchange(core_sum, XY)
    plane_sum = second[:, : shards * 32].astype(f32).sum(axis=0).astype(bf16)
    half_grad = second[:, shards * 32 :].astype(f32).sum(axis=0)
    total_grad = (half_grad + swapped(half_grad, "zh")).astype(bf16)
    for_z = jnp.broadcast_to(plane_sum.reshape(1, shards, 32, 128), (2, shards, 32, 128))
    third = exchange(for_z.reshape(2 * shards, 32, 128), ZZ)
    tower_sum = third.astype(f32).sum(axis=0).astype(bf16)
    own = to_all(jnp.concatenate([tower_sum, total_grad], axis=0), XY)
    other = swapped(own, "core")

    tower_scale = 1.0 / math.sqrt(tok * shards * lax.axis_size(DP))
    new_table, new_accum, gate_sum, up_sum = update(own, other, table, accum, tower_scale)
    return (new_table, new_accum, gate_sum, up_sum, emb_grad)


def solution(mesh):
    torus = Mesh(mesh.devices.reshape(4, 4, 2, 2, mesh.shape["emb"]), DP_EMB)
    return jax.shard_map(
        step,
        mesh=torus,
        in_specs=(
            P(DP_EMB),
            P(DP_EMB),
            P(DP_EMB, None),
            P(),
            P("emb", None),
            P("emb", None),
            P(DP),
            P(),
            P(None, "emb"),
            P(None, "emb"),
            P("emb"),
        ),
        out_specs=(P("emb", None), P("emb", None), P(None, "emb"), P(None, "emb"), P(DP_EMB, None)),
        check_vma=False,
    )
```

```python
import math

import jax
import jax.numpy as jnp
from jax import lax
from jax.experimental import pallas as pl
from jax.experimental.pallas import tpu as pltpu
from jax.sharding import Mesh
from jax.sharding import PartitionSpec as P


DP = ("x", "y", "zh", "core")
DP_EMB = ("x", "y", "zh", "core", "emb")
XY = ("x", "y")
ZZ = ("zh", "emb")


loss_weight = 64.0
learn_rate = 0.1
norm_eps = 1e-06

bf16 = jnp.bfloat16
f32 = jnp.float32


def exchange(pieces, axis):
    return lax.all_to_all(pieces, axis, 0, 0, tiled=True)


def to_all(array, axis):
    return exchange(jnp.broadcast_to(array[None], (lax.axis_size(axis), *array.shape)), axis)


def dot32(a, b):
    return jnp.dot(a, b, preferred_element_type=f32)


def packed(ids, parts, capacity, shards, rows_shard):
    tok = ids.shape[1]
    lines = parts.shape[0]
    row = lax.broadcasted_iota(jnp.int32, (lines, tok), 0)
    pick = jnp.where(ids // 128 == row, 1.0, 0.0).astype(bf16)
    found = lax.dot_general(parts, pick, (((0,), (0,)), ((), ())), preferred_element_type=f32)
    lane = lax.broadcasted_iota(jnp.int32, (128, tok), 0) == ids % 128
    high = jnp.sum(jnp.where(lane, found[:128], 0.0), axis=0, keepdims=True)
    low = jnp.sum(jnp.where(lane, found[128:], 0.0), axis=0, keepdims=True)
    place = (high * 128.0 + low).astype(jnp.int32)
    shard = lax.broadcasted_iota(jnp.int32, (shards, tok), 0)
    match = (place >= shard * rows_shard) & (place < (shard + 1) * rows_shard)
    matched = jnp.where(match, 1.0, 0.0)
    owner = jnp.sum(jnp.where(match, shard, 0), axis=0, keepdims=True)
    slot = place - owner * rows_shard
    earlier = lax.broadcasted_iota(jnp.int32, (tok, tok), 0) <= lax.broadcasted_iota(
        jnp.int32, (tok, tok), 1
    )
    counts = dot32(matched.astype(bf16), jnp.where(earlier, 1.0, 0.0).astype(bf16))
    rank = jnp.sum(matched * counts, axis=0, keepdims=True).astype(jnp.int32) - 1
    line = lax.broadcasted_iota(jnp.int32, (128, tok), 0)
    spread = jnp.where(line % capacity == rank, 1.0, 0.0).astype(bf16)
    both = (((1,), (1,)), ((), ()))
    codes = [
        lax.dot_general(
            (matched * part.astype(f32)).astype(bf16), spread, both, preferred_element_type=f32
        )
        for part in (slot // 128 + 1, slot % 128)
    ]
    first_half = lax.broadcasted_iota(jnp.int32, (shards, 128), 1) < capacity
    code = jnp.where(first_half, codes[0], codes[1])
    return code, owner * capacity + rank


def pack_kernel(*refs, capacity, rows_shard):
    sources, (out_ref, pos_ref), buffers, sems = refs[:7], refs[7:9], refs[9:16], refs[16]
    copies = [
        pltpu.make_async_copy(source, buffer, sems.at[i])
        for i, (source, buffer) in enumerate(zip(sources, buffers, strict=True))
    ]
    for i in (0, 1, 3, 2, 4, 5, 6):
        copies[i].start()
    for i in (0, 1, 3):
        copies[i].wait()
    cur_ref, prev_ref, grads_ref, places_ref, w_gate_ref, w_up_ref, w_out_ref = buffers
    shards = out_ref.shape[0]
    places = places_ref[...]
    parts = jnp.concatenate(
        [(places // 128).astype(f32), (places % 128).astype(f32)], axis=1
    ).astype(bf16)
    cur_code, cur_pos = packed(cur_ref[...], parts, capacity, shards, rows_shard)
    prev_code, prev_pos = packed(prev_ref[...], parts, capacity, shards, rows_shard)
    pos_ref[...] = cur_pos
    slots = shards * capacity
    slot_row = lax.broadcasted_iota(jnp.int32, (slots, prev_pos.shape[1]), 0)
    pack = jnp.where(slot_row == prev_pos, 1.0, 0.0).astype(bf16)
    for i in (2, 4, 5, 6):
        copies[i].wait()
    rows = dot32(pack, grads_ref[...]).astype(bf16)
    at = lax.axis_index(XY)
    cut = (pl.ds(pl.multiple_of((at % 4) * 32, 32), 32), pl.ds(pl.multiple_of((at // 4) * 128, 128), 128))
    gate_slice = w_gate_ref[cut].astype(f32)
    up_slice = w_up_ref[cut].astype(f32)
    own = jnp.where(lax.axis_index("core") == 0, gate_slice, up_slice).astype(bf16)
    out = jnp.concatenate([w_out_ref[...].astype(f32), jnp.zeros((12, 128), f32)], axis=0)
    tail_row = lax.broadcasted_iota(jnp.int32, (16, 128), 0)
    for shard in range(shards):
        out_ref[shard, :capacity, :] = rows[shard * capacity : (shard + 1) * capacity]
        out_ref[shard, capacity : capacity + 32, :] = own
        tail = jnp.where(tail_row == 14, cur_code[shard : shard + 1], out)
        tail = jnp.where(tail_row == 15, prev_code[shard : shard + 1], tail)
        out_ref[shard, capacity + 32 : capacity + 48, :] = tail.astype(bf16)


def pack(cur_ids, prev_ids, prev_grads, row_place, w_gate, w_up, w_out, shards, capacity, rows_shard):
    vmem = pl.BlockSpec(memory_space=pltpu.VMEM)
    tok = cur_ids.shape[0]
    arrays = (
        cur_ids.reshape(1, tok), prev_ids.reshape(1, tok), prev_grads,
        row_place.reshape(-1, 128), w_gate, w_up, w_out.reshape(4, 128),
    )
    return pl.pallas_call(
        lambda *refs: pack_kernel(*refs, capacity=capacity, rows_shard=rows_shard),
        out_shape=(
            jax.ShapeDtypeStruct((shards, capacity + 48, 128), bf16),
            jax.ShapeDtypeStruct((1, tok), jnp.int32),
        ),
        in_specs=[pl.BlockSpec(memory_space=pltpu.HBM)] * len(arrays),
        out_specs=(vmem, vmem),
        scratch_shapes=[pltpu.VMEM(array.shape, array.dtype) for array in arrays]
        + [pltpu.SemaphoreType.DMA((len(arrays),))],
        compiler_params=pltpu.CompilerParams(vmem_limit_bytes=62 * 1024 * 1024),
        name="pack",
    )(*arrays)


def decoded(line, capacity):
    values = line.astype(jnp.int32)
    return ((values[..., :capacity] - 1) * 128 + values[..., capacity:]).reshape(-1)


def tower_kernel(
    answers_ref, target_ref, own_ref, other_ref, w_gate_ref, w_up_ref, shared_ref,
    gain_ref, labels_ref, table_part_ref, emb_grad_ref, grads_ref, weights_s, gate_s, up_s,
):
    tok = target_ref.shape[1]
    width = answers_ref.shape[1]
    shards, span = shared_ref.shape[:2]
    lines = own_ref.shape[0] // 16
    core = lax.axis_index("core")
    home = lax.axis_index("emb")
    weights_s[core] = own_ref[...]
    weights_s[1 - core] = other_ref[...]
    slot_row = lax.broadcasted_iota(jnp.int32, (answers_ref.shape[0], tok), 0)
    pick = jnp.where(target_ref[...] == slot_row, 1.0, 0.0).astype(bf16)
    values = lax.dot_general(
        pick, answers_ref[...], (((0,), (0,)), ((), ())), preferred_element_type=f32
    )
    turned = labels_ref[...].T
    mine = lax.broadcasted_iota(jnp.int32, turned.shape, 1) == home
    targets = jnp.sum(jnp.where(mine, turned, 0.0), axis=1, keepdims=True)
    inverse_rms = lax.rsqrt(jnp.mean(values * values, axis=1, keepdims=True) + norm_eps)
    gain = gain_ref[...]
    normed_wide = values * inverse_rms * gain
    normed = normed_wide.astype(bf16)
    normed_t = normed_wide.T.astype(bf16)

    column = lax.axis_index("x")

    def far_block(hop, half, side):
        tiles = []
        for tile in (2 * half, 2 * half + 1):
            turn = (tile - column + 4) % 4
            quarters = [
                weights_s[side, pl.ds(pl.multiple_of((k * 4 + turn) * lines + hop * 32, 32), 32), :]
                for k in range(4)
            ]
            tiles.append(jnp.concatenate(quarters, axis=0))
        return jnp.concatenate(tiles, axis=1)

    def home_block(hop, half, side):
        return (w_gate_ref, w_up_ref)[side][:, half * 256 : (half + 1) * 256]

    def out_row(shard, half, j):
        return shared_ref[shard, pl.ds(span - 16 + 2 * half + j, 1), :].astype(f32)

    def forward(hop, total, block):
        shard = (home + 1 + hop) % shards
        for half in range(2):
            at = hop * 2 + half
            gate = dot32(normed, block(hop, half, 0))
            up = dot32(normed, block(hop, half, 1))
            sig = jax.nn.sigmoid(gate)
            act = gate * sig
            gate_s[at] = up * (sig + act * (1.0 - sig))
            up_s[at] = act
            hidden = (act * up).astype(bf16).astype(f32)
            for j in range(2):
                total = total + hidden[:, j * 128 : (j + 1) * 128] * out_row(shard, half, j)
        return total

    total = forward(shards - 1, jnp.zeros((tok, 128), f32), home_block)
    total = lax.fori_loop(0, shards - 1, lambda hop, t: forward(hop, t, far_block), total, unroll=True)
    logits = jnp.sum(total, axis=1, keepdims=True)
    slopes = loss_weight * (jax.nn.sigmoid(logits) - targets)

    across = (((1,), (1,)), ((), ()))

    def backward(hop, back, block):
        shard = (home + 1 + hop) % shards
        for half in range(2):
            at = hop * 2 + half
            out = jnp.concatenate([out_row(shard, half, j) for j in range(2)], axis=1)
            back_hidden = slopes * out
            back_gate = (back_hidden * gate_s[at]).astype(bf16)
            back_up = (back_hidden * up_s[at]).astype(bf16)
            for side, part in ((0, back_gate), (1, back_up)):
                back = back + lax.dot_general(
                    part, block(hop, half, side), across, preferred_element_type=f32
                )
                grad = dot32(normed_t, part).astype(bf16)
                place = core if side == 0 else 1 - core
                for j in range(2):
                    tile = 2 * half + j
                    for k in range(4):
                        grads_ref[
                            place, tile * 4 + k, pl.ds(shard * 32, 32), :
                        ] = grad[k * 32 : (k + 1) * 32, j * 128 : (j + 1) * 128]
        return back

    back = backward(shards - 1, jnp.zeros((tok, width), f32), home_block)
    back = lax.fori_loop(0, shards - 1, lambda hop, b: backward(hop, b, far_block), back, unroll=True)
    grads_ref[:, :, shards * 32 :, :] = table_part_ref[...]
    scaled = back * gain
    emb_grad_ref[...] = inverse_rms * scaled - values * (
        inverse_rms * inverse_rms * inverse_rms
    ) * jnp.mean(values * scaled, axis=1, keepdims=True)


def tower(answers, target, own, other, w_gate, w_up, shared, gain, labels, table_part):
    tok = target.shape[1]
    width = answers.shape[1]
    shards = shared.shape[0]
    vmem = pl.BlockSpec(memory_space=pltpu.VMEM)
    return pl.pallas_call(
        tower_kernel,
        out_shape=(
            jax.ShapeDtypeStruct((tok, width), f32),
            jax.ShapeDtypeStruct((2, 16, shards * 32 + table_part.shape[2], width), bf16),
        ),
        in_specs=[vmem] * 10,
        out_specs=(vmem, vmem),
        scratch_shapes=[pltpu.VMEM((2, *own.shape), bf16)]
        + [pltpu.VMEM((2 * shards, tok, 256), f32)] * 2,
        compiler_params=pltpu.CompilerParams(vmem_limit_bytes=20 * 1024 * 1024),
        cost_estimate=pl.CostEstimate(
            flops=6 * 2 * tok * width * 4096, bytes_accessed=5 << 20, transcendentals=2 << 20
        ),
        name="tower",
    )(
        answers, target, own, other, w_gate, w_up, shared,
        gain.reshape(1, -1), labels.reshape(shards, tok), table_part,
    )


def update_kernel(
    own_ref, other_ref, table_ref, accum_ref,
    new_table_ref, new_accum_ref, gate_ref, up_ref, both_s, *, scale,
):
    core = lax.axis_index("core")
    both_s[core] = own_ref[...]
    both_s[1 - core] = other_ref[...]
    plane, lines = own_ref.shape[:2]
    span = lines - 32
    for side, out_ref in ((0, gate_ref), (1, up_ref)):
        for q in range(plane):
            tile, k = q // 4, q % 4
            out_ref[k * 32 : (k + 1) * 32, tile * 128 : (tile + 1) * 128] = (
                both_s[side, q, :32, :].astype(f32) * scale
            )
            rows = pl.ds((2 * q + side) * span, span)
            grad = both_s[side, q, 32:, :].astype(f32)
            total = accum_ref[rows, :] + grad * grad
            new_accum_ref[rows, :] = total
            new_table_ref[rows, :] = table_ref[rows, :] - learn_rate * grad * lax.rsqrt(total)


def update(own, other, table, accum, scale):
    vmem = pl.BlockSpec(memory_space=pltpu.VMEM)
    part = jax.ShapeDtypeStruct((128, 512), f32)
    return pl.pallas_call(
        lambda *refs: update_kernel(*refs, scale=scale),
        out_shape=(
            jax.ShapeDtypeStruct(table.shape, f32),
            jax.ShapeDtypeStruct(table.shape, f32),
            part,
            part,
        ),
        in_specs=[vmem] * 4,
        out_specs=(vmem,) * 4,
        scratch_shapes=[pltpu.VMEM((2, *own.shape), bf16)],
        compiler_params=pltpu.CompilerParams(vmem_limit_bytes=12 * 1024 * 1024),
        name="update",
    )(own, other, table, accum)


def swapped(array, axis):
    return lax.ppermute(array, axis, [(0, 1), (1, 0)])


def step(
    cur_ids, prev_ids, prev_grads, row_place, table, accum, labels, gain, w_gate, w_up, w_out
):
    shards = lax.axis_size("emb")
    plane = lax.axis_size(XY)
    rows_shard, width = table.shape
    tok = cur_ids.shape[0]
    capacity = min(tok, 2 * tok // shards)
    slots = shards * capacity
    core = lax.axis_index("core")
    home = lax.axis_index("emb")
    payload, cur_pos = pack(
        cur_ids, prev_ids, prev_grads, row_place, w_gate, w_up, w_out,
        shards, capacity, rows_shard,
    )
    first = exchange(payload, "emb")
    rows_table = lax.optimization_barrier(table.astype(bf16))
    got_rows = first[:, :capacity].reshape(slots, width)
    slices = first[:, capacity : capacity + 32]
    wanted = decoded(first[:, capacity + 46], capacity)
    got_slots = decoded(first[:, capacity + 47], capacity)

    row_ids = jnp.arange(rows_shard, dtype=jnp.int32)
    fetched = dot32(
        (wanted[:, None] == row_ids[None, :]).astype(bf16), rows_table
    ).astype(bf16)
    answers = exchange(fetched.reshape(shards, capacity, width), "emb").reshape(slots, width)

    span = rows_shard // plane // 2
    half_ids = jnp.arange(rows_shard // 2, dtype=jnp.int32)
    half_ids = half_ids // span * (2 * span) + half_ids % span
    part_ids = jnp.concatenate([half_ids + core * span, half_ids + (1 - core) * span])
    table_part = dot32((part_ids[:, None] == got_slots[None, :]).astype(bf16), got_rows)
    table_part = table_part.astype(bf16).reshape(2, plane, span, width)

    foreign = lax.dynamic_slice(
        jnp.concatenate([slices, slices], axis=0), (home + 1, 0, 0), (shards - 1, 32, 128)
    ).reshape((shards - 1) * 32, 128)
    ring = lax.axis_size("x")
    turns = [foreign]
    for step in range(1, ring):
        turns.append(lax.ppermute(foreign, "x", [(i, (i - step) % ring) for i in range(ring)]))
    own_weights = lax.all_gather(jnp.concatenate(turns, axis=0), "y", axis=0, tiled=True)
    other_weights = swapped(own_weights, "core")
    emb_grad, tower_grads = tower(
        answers, cur_pos, own_weights, other_weights, w_gate, w_up, first, gain, labels,
        table_part,
    )

    received = swapped(tower_grads[1], "core")
    core_sum = (tower_grads[0].astype(f32) + received.astype(f32)).astype(bf16)
    second = exchange(core_sum, XY)
    plane_sum = second[:, : shards * 32].astype(f32).sum(axis=0).astype(bf16)
    half_grad = second[:, shards * 32 :].astype(f32).sum(axis=0)
    total_grad = (half_grad + swapped(half_grad, "zh")).astype(bf16)
    for_z = jnp.broadcast_to(plane_sum.reshape(1, shards, 32, 128), (2, shards, 32, 128))
    third = exchange(for_z.reshape(2 * shards, 32, 128), ZZ)
    tower_sum = third.astype(f32).sum(axis=0).astype(bf16)
    own = to_all(jnp.concatenate([tower_sum, total_grad], axis=0), XY)
    other = swapped(own, "core")

    tower_scale = 1.0 / math.sqrt(tok * shards * lax.axis_size(DP))
    new_table, new_accum, gate_sum, up_sum = update(own, other, table, accum, tower_scale)
    return (new_table, new_accum, gate_sum, up_sum, emb_grad)


def solution(mesh):
    torus = Mesh(mesh.devices.reshape(4, 4, 2, 2, mesh.shape["emb"]), DP_EMB)
    return jax.shard_map(
        step,
        mesh=torus,
        in_specs=(
            P(DP_EMB),
            P(DP_EMB),
            P(DP_EMB, None),
            P(),
            P("emb", None),
            P("emb", None),
            P(DP),
            P(),
            P(None, "emb"),
            P(None, "emb"),
            P("emb"),
        ),
        out_specs=(P("emb", None), P("emb", None), P(None, "emb"), P(None, "emb"), P(DP_EMB, None)),
        check_vma=False,
    )
```

```python
import math

import jax
import jax.numpy as jnp
from jax import lax
from jax.experimental import pallas as pl
from jax.experimental.pallas import tpu as pltpu
from jax.sharding import Mesh
from jax.sharding import PartitionSpec as P


DP = ("x", "y", "zh", "core")
DP_EMB = ("x", "y", "zh", "core", "emb")
XY = ("x", "y")
ZZ = ("zh", "emb")


loss_weight = 64.0
learn_rate = 0.1
norm_eps = 1e-06

bf16 = jnp.bfloat16
f32 = jnp.float32


def exchange(pieces, axis):
    return lax.all_to_all(pieces, axis, 0, 0, tiled=True)


def to_all(array, axis):
    return exchange(jnp.broadcast_to(array[None], (lax.axis_size(axis), *array.shape)), axis)


def dot32(a, b):
    return jnp.dot(a, b, preferred_element_type=f32)


def packed(ids, parts, capacity, shards, rows_shard):
    tok = ids.shape[1]
    lines = parts.shape[0]
    row = lax.broadcasted_iota(jnp.int32, (lines, tok), 0)
    pick = jnp.where(ids // 128 == row, 1.0, 0.0).astype(bf16)
    found = lax.dot_general(parts, pick, (((0,), (0,)), ((), ())), preferred_element_type=f32)
    lane = lax.broadcasted_iota(jnp.int32, (128, tok), 0) == ids % 128
    high = jnp.sum(jnp.where(lane, found[:128], 0.0), axis=0, keepdims=True)
    low = jnp.sum(jnp.where(lane, found[128:], 0.0), axis=0, keepdims=True)
    place = (high * 128.0 + low).astype(jnp.int32)
    shard = lax.broadcasted_iota(jnp.int32, (shards, tok), 0)
    match = (place >= shard * rows_shard) & (place < (shard + 1) * rows_shard)
    matched = jnp.where(match, 1.0, 0.0)
    owner = jnp.sum(jnp.where(match, shard, 0), axis=0, keepdims=True)
    slot = place - owner * rows_shard
    earlier = lax.broadcasted_iota(jnp.int32, (tok, tok), 0) <= lax.broadcasted_iota(
        jnp.int32, (tok, tok), 1
    )
    counts = dot32(matched.astype(bf16), jnp.where(earlier, 1.0, 0.0).astype(bf16))
    rank = jnp.sum(matched * counts, axis=0, keepdims=True).astype(jnp.int32) - 1
    line = lax.broadcasted_iota(jnp.int32, (128, tok), 0)
    spread = jnp.where(line % capacity == rank, 1.0, 0.0).astype(bf16)
    both = (((1,), (1,)), ((), ()))
    codes = [
        lax.dot_general(
            (matched * part.astype(f32)).astype(bf16), spread, both, preferred_element_type=f32
        )
        for part in (slot // 128 + 1, slot % 128)
    ]
    first_half = lax.broadcasted_iota(jnp.int32, (shards, 128), 1) < capacity
    code = jnp.where(first_half, codes[0], codes[1])
    return code, owner * capacity + rank


def pack_kernel(*refs, capacity, rows_shard):
    sources, (out_ref, pos_ref), buffers, sems = refs[:7], refs[7:9], refs[9:16], refs[16]
    copies = [
        pltpu.make_async_copy(source, buffer, sems.at[i])
        for i, (source, buffer) in enumerate(zip(sources, buffers, strict=True))
    ]
    for i in (0, 1, 3, 2, 4, 5, 6):
        copies[i].start()
    for i in (0, 1, 3):
        copies[i].wait()
    cur_ref, prev_ref, grads_ref, places_ref, w_gate_ref, w_up_ref, w_out_ref = buffers
    shards = out_ref.shape[0]
    places = places_ref[...]
    parts = jnp.concatenate(
        [(places // 128).astype(f32), (places % 128).astype(f32)], axis=1
    ).astype(bf16)
    cur_code, cur_pos = packed(cur_ref[...], parts, capacity, shards, rows_shard)
    prev_code, prev_pos = packed(prev_ref[...], parts, capacity, shards, rows_shard)
    pos_ref[...] = cur_pos
    slots = shards * capacity
    slot_row = lax.broadcasted_iota(jnp.int32, (slots, prev_pos.shape[1]), 0)
    pack = jnp.where(slot_row == prev_pos, 1.0, 0.0).astype(bf16)
    for i in (2, 4, 5, 6):
        copies[i].wait()
    rows = dot32(pack, grads_ref[...]).astype(bf16)
    at = lax.axis_index(XY)
    cut = (pl.ds(pl.multiple_of((at % 4) * 32, 32), 32), pl.ds(pl.multiple_of((at // 4) * 128, 128), 128))
    gate_slice = w_gate_ref[cut].astype(f32)
    up_slice = w_up_ref[cut].astype(f32)
    own = jnp.where(lax.axis_index("core") == 0, gate_slice, up_slice).astype(bf16)
    out = jnp.concatenate([w_out_ref[...].astype(f32), jnp.zeros((12, 128), f32)], axis=0)
    tail_row = lax.broadcasted_iota(jnp.int32, (16, 128), 0)
    for shard in range(shards):
        out_ref[shard, :capacity, :] = rows[shard * capacity : (shard + 1) * capacity]
        out_ref[shard, capacity : capacity + 32, :] = own
        tail = jnp.where(tail_row == 14, cur_code[shard : shard + 1], out)
        tail = jnp.where(tail_row == 15, prev_code[shard : shard + 1], tail)
        out_ref[shard, capacity + 32 : capacity + 48, :] = tail.astype(bf16)


def pack(cur_ids, prev_ids, prev_grads, row_place, w_gate, w_up, w_out, shards, capacity, rows_shard):
    vmem = pl.BlockSpec(memory_space=pltpu.VMEM)
    tok = cur_ids.shape[0]
    arrays = (
        cur_ids.reshape(1, tok), prev_ids.reshape(1, tok), prev_grads,
        row_place.reshape(-1, 128), w_gate, w_up, w_out.reshape(4, 128),
    )
    return pl.pallas_call(
        lambda *refs: pack_kernel(*refs, capacity=capacity, rows_shard=rows_shard),
        out_shape=(
            jax.ShapeDtypeStruct((shards, capacity + 48, 128), bf16),
            jax.ShapeDtypeStruct((1, tok), jnp.int32),
        ),
        in_specs=[pl.BlockSpec(memory_space=pltpu.HBM)] * len(arrays),
        out_specs=(vmem, vmem),
        scratch_shapes=[pltpu.VMEM(array.shape, array.dtype) for array in arrays]
        + [pltpu.SemaphoreType.DMA((len(arrays),))],
        compiler_params=pltpu.CompilerParams(vmem_limit_bytes=62 * 1024 * 1024),
        name="pack",
    )(*arrays)


def decoded(line, capacity):
    values = line.astype(jnp.int32)
    return ((values[..., :capacity] - 1) * 128 + values[..., capacity:]).reshape(-1)


def tower_kernel(
    answers_ref, target_ref, own_ref, other_ref, w_gate_ref, w_up_ref, shared_ref,
    gain_ref, labels_ref, table_part_ref, emb_grad_ref, grads_ref, weights_s, gate_s, up_s,
):
    tok = target_ref.shape[1]
    width = answers_ref.shape[1]
    shards, span = shared_ref.shape[:2]
    lines = own_ref.shape[0] // 16
    core = lax.axis_index("core")
    home = lax.axis_index("emb")
    weights_s[core] = own_ref[...]
    weights_s[1 - core] = other_ref[...]
    slot_row = lax.broadcasted_iota(jnp.int32, (answers_ref.shape[0], tok), 0)
    pick = jnp.where(target_ref[...] == slot_row, 1.0, 0.0).astype(bf16)
    values = lax.dot_general(
        pick, answers_ref[...], (((0,), (0,)), ((), ())), preferred_element_type=f32
    )
    turned = labels_ref[...].T
    mine = lax.broadcasted_iota(jnp.int32, turned.shape, 1) == home
    targets = jnp.sum(jnp.where(mine, turned, 0.0), axis=1, keepdims=True)
    inverse_rms = lax.rsqrt(jnp.mean(values * values, axis=1, keepdims=True) + norm_eps)
    gain = gain_ref[...]
    normed_wide = values * inverse_rms * gain
    normed = normed_wide.astype(bf16)
    normed_t = normed_wide.T.astype(bf16)

    def far_block(hop, half, side):
        tiles = []
        for tile in (2 * half, 2 * half + 1):
            quarters = [
                weights_s[side, pl.ds((k * 4 + tile) * lines + hop * 32, 32), :]
                for k in range(4)
            ]
            tiles.append(jnp.concatenate(quarters, axis=0))
        return jnp.concatenate(tiles, axis=1)

    def home_block(hop, half, side):
        return (w_gate_ref, w_up_ref)[side][:, half * 256 : (half + 1) * 256]

    def out_row(shard, half, j):
        return shared_ref[shard, pl.ds(span - 16 + 2 * half + j, 1), :].astype(f32)

    def forward(hop, total, block):
        shard = (home + 1 + hop) % shards
        for half in range(2):
            at = hop * 2 + half
            gate = dot32(normed, block(hop, half, 0))
            up = dot32(normed, block(hop, half, 1))
            sig = jax.nn.sigmoid(gate)
            act = gate * sig
            gate_s[at] = up * (sig + act * (1.0 - sig))
            up_s[at] = act
            hidden = (act * up).astype(bf16).astype(f32)
            for j in range(2):
                total = total + hidden[:, j * 128 : (j + 1) * 128] * out_row(shard, half, j)
        return total

    total = forward(shards - 1, jnp.zeros((tok, 128), f32), home_block)
    total = lax.fori_loop(0, shards - 1, lambda hop, t: forward(hop, t, far_block), total, unroll=True)
    logits = jnp.sum(total, axis=1, keepdims=True)
    slopes = loss_weight * (jax.nn.sigmoid(logits) - targets)

    across = (((1,), (1,)), ((), ()))

    def backward(hop, back, block):
        shard = (home + 1 + hop) % shards
        for half in range(2):
            at = hop * 2 + half
            out = jnp.concatenate([out_row(shard, half, j) for j in range(2)], axis=1)
            back_hidden = slopes * out
            back_gate = (back_hidden * gate_s[at]).astype(bf16)
            back_up = (back_hidden * up_s[at]).astype(bf16)
            for side, part in ((0, back_gate), (1, back_up)):
                back = back + lax.dot_general(
                    part, block(hop, half, side), across, preferred_element_type=f32
                )
                grad = dot32(normed_t, part).astype(bf16)
                place = core if side == 0 else 1 - core
                for j in range(2):
                    tile = 2 * half + j
                    for k in range(4):
                        grads_ref[
                            place, tile * 4 + k, pl.ds(shard * 32, 32), :
                        ] = grad[k * 32 : (k + 1) * 32, j * 128 : (j + 1) * 128]
        return back

    back = backward(shards - 1, jnp.zeros((tok, width), f32), home_block)
    back = lax.fori_loop(0, shards - 1, lambda hop, b: backward(hop, b, far_block), back, unroll=True)
    grads_ref[:, :, shards * 32 :, :] = table_part_ref[...]
    scaled = back * gain
    emb_grad_ref[...] = inverse_rms * scaled - values * (
        inverse_rms * inverse_rms * inverse_rms
    ) * jnp.mean(values * scaled, axis=1, keepdims=True)


def tower(answers, target, own, other, w_gate, w_up, shared, gain, labels, table_part):
    tok = target.shape[1]
    width = answers.shape[1]
    shards = shared.shape[0]
    vmem = pl.BlockSpec(memory_space=pltpu.VMEM)
    return pl.pallas_call(
        tower_kernel,
        out_shape=(
            jax.ShapeDtypeStruct((tok, width), f32),
            jax.ShapeDtypeStruct((2, 16, shards * 32 + table_part.shape[2], width), bf16),
        ),
        in_specs=[vmem] * 10,
        out_specs=(vmem, vmem),
        scratch_shapes=[pltpu.VMEM((2, *own.shape), bf16)]
        + [pltpu.VMEM((2 * shards, tok, 256), f32)] * 2,
        compiler_params=pltpu.CompilerParams(vmem_limit_bytes=20 * 1024 * 1024),
        cost_estimate=pl.CostEstimate(
            flops=6 * 2 * tok * width * 4096, bytes_accessed=5 << 20, transcendentals=2 << 20
        ),
        name="tower",
    )(
        answers, target, own, other, w_gate, w_up, shared,
        gain.reshape(1, -1), labels.reshape(shards, tok), table_part,
    )


def update_kernel(
    own_ref, other_ref, table_ref, accum_ref,
    new_table_ref, new_accum_ref, gate_ref, up_ref, both_s, *, scale,
):
    core = lax.axis_index("core")
    both_s[core] = own_ref[...]
    both_s[1 - core] = other_ref[...]
    plane, lines = own_ref.shape[:2]
    span = lines - 32
    for side, out_ref in ((0, gate_ref), (1, up_ref)):
        for q in range(plane):
            tile, k = q // 4, q % 4
            out_ref[k * 32 : (k + 1) * 32, tile * 128 : (tile + 1) * 128] = (
                both_s[side, q, :32, :].astype(f32) * scale
            )
            rows = pl.ds((2 * q + side) * span, span)
            grad = both_s[side, q, 32:, :].astype(f32)
            total = accum_ref[rows, :] + grad * grad
            new_accum_ref[rows, :] = total
            new_table_ref[rows, :] = table_ref[rows, :] - learn_rate * grad * lax.rsqrt(total)


def update(own, other, table, accum, scale):
    vmem = pl.BlockSpec(memory_space=pltpu.VMEM)
    part = jax.ShapeDtypeStruct((128, 512), f32)
    return pl.pallas_call(
        lambda *refs: update_kernel(*refs, scale=scale),
        out_shape=(
            jax.ShapeDtypeStruct(table.shape, f32),
            jax.ShapeDtypeStruct(table.shape, f32),
            part,
            part,
        ),
        in_specs=[vmem] * 4,
        out_specs=(vmem,) * 4,
        scratch_shapes=[pltpu.VMEM((2, *own.shape), bf16)],
        compiler_params=pltpu.CompilerParams(vmem_limit_bytes=12 * 1024 * 1024),
        name="update",
    )(own, other, table, accum)


def swapped(array, axis):
    return lax.ppermute(array, axis, [(0, 1), (1, 0)])


def step(
    cur_ids, prev_ids, prev_grads, row_place, table, accum, labels, gain, w_gate, w_up, w_out
):
    shards = lax.axis_size("emb")
    plane = lax.axis_size(XY)
    rows_shard, width = table.shape
    tok = cur_ids.shape[0]
    capacity = min(tok, 2 * tok // shards)
    slots = shards * capacity
    core = lax.axis_index("core")
    home = lax.axis_index("emb")
    payload, cur_pos = pack(
        cur_ids, prev_ids, prev_grads, row_place, w_gate, w_up, w_out,
        shards, capacity, rows_shard,
    )
    first = exchange(payload, "emb")
    rows_table = lax.optimization_barrier(table.astype(bf16))
    got_rows = first[:, :capacity].reshape(slots, width)
    slices = first[:, capacity : capacity + 32]
    wanted = decoded(first[:, capacity + 46], capacity)
    got_slots = decoded(first[:, capacity + 47], capacity)

    row_ids = jnp.arange(rows_shard, dtype=jnp.int32)
    hot = (wanted[:, None] == row_ids[None, :]).astype(bf16)
    fetched = dot32(hot, rows_table).astype(bf16)
    span = rows_shard // plane // 2
    half_ids = jnp.arange(rows_shard // 2, dtype=jnp.int32)
    half_ids = half_ids // span * (2 * span) + half_ids % span
    part_ids = jnp.concatenate([half_ids + core * span, half_ids + (1 - core) * span])
    table_part = dot32((part_ids[:, None] == got_slots[None, :]).astype(bf16), got_rows)
    table_part = table_part.astype(bf16).reshape(2, plane, span, width)

    foreign = lax.dynamic_slice(
        jnp.concatenate([slices, slices], axis=0), (home + 1, 0, 0), (shards - 1, 32, 128)
    ).reshape((shards - 1) * 32, 128)
    column = to_all(foreign, "x")
    column, fetched = lax.optimization_barrier((column, fetched))
    answers = exchange(fetched.reshape(shards, capacity, width), "emb").reshape(slots, width)
    own_weights = lax.all_gather(column.reshape(-1, 128), "y", axis=0, tiled=True)
    other_weights = swapped(own_weights, "core")
    emb_grad, tower_grads = tower(
        answers, cur_pos, own_weights, other_weights, w_gate, w_up, first, gain, labels,
        table_part,
    )

    received = swapped(tower_grads[1], "core")
    core_sum = (tower_grads[0].astype(f32) + received.astype(f32)).astype(bf16)
    second = exchange(core_sum, XY)
    plane_sum = second[:, : shards * 32].astype(f32).sum(axis=0).astype(bf16)
    half_grad = second[:, shards * 32 :].astype(f32).sum(axis=0)
    total_grad = (half_grad + swapped(half_grad, "zh")).astype(bf16)
    for_z = jnp.broadcast_to(plane_sum.reshape(1, shards, 32, 128), (2, shards, 32, 128))
    third = exchange(for_z.reshape(2 * shards, 32, 128), ZZ)
    tower_sum = third.astype(f32).sum(axis=0).astype(bf16)
    own = to_all(jnp.concatenate([tower_sum, total_grad], axis=0), XY)
    other = swapped(own, "core")

    tower_scale = 1.0 / math.sqrt(tok * shards * lax.axis_size(DP))
    new_table, new_accum, gate_sum, up_sum = update(own, other, table, accum, tower_scale)
    return (new_table, new_accum, gate_sum, up_sum, emb_grad)


def solution(mesh):
    torus = Mesh(mesh.devices.reshape(4, 4, 2, 2, mesh.shape["emb"]), DP_EMB)
    return jax.shard_map(
        step,
        mesh=torus,
        in_specs=(
            P(DP_EMB),
            P(DP_EMB),
            P(DP_EMB, None),
            P(),
            P("emb", None),
            P("emb", None),
            P(DP),
            P(),
            P(None, "emb"),
            P(None, "emb"),
            P("emb"),
        ),
        out_specs=(P("emb", None), P("emb", None), P(None, "emb"), P(None, "emb"), P(DP_EMB, None)),
        check_vma=False,
    )
```

```python
import math

import jax
import jax.numpy as jnp
from jax import lax
from jax.experimental import pallas as pl
from jax.experimental.pallas import tpu as pltpu
from jax.sharding import Mesh
from jax.sharding import PartitionSpec as P


DP = ("x", "y", "zh", "core")
DP_EMB = ("x", "y", "zh", "core", "emb")
XY = ("x", "y")
ZZ = ("zh", "emb")


loss_weight = 64.0
learn_rate = 0.1
norm_eps = 1e-06

bf16 = jnp.bfloat16
f32 = jnp.float32


def exchange(pieces, axis):
    return lax.all_to_all(pieces, axis, 0, 0, tiled=True)


def to_all(array, axis):
    return exchange(jnp.broadcast_to(array[None], (lax.axis_size(axis), *array.shape)), axis)


def dot32(a, b):
    return jnp.dot(a, b, preferred_element_type=f32)


def packed(ids, parts, capacity, shards, rows_shard):
    tok = ids.shape[1]
    lines = parts.shape[0]
    row = lax.broadcasted_iota(jnp.int32, (lines, tok), 0)
    pick = jnp.where(ids // 128 == row, 1.0, 0.0).astype(bf16)
    found = lax.dot_general(parts, pick, (((0,), (0,)), ((), ())), preferred_element_type=f32)
    lane = lax.broadcasted_iota(jnp.int32, (128, tok), 0) == ids % 128
    high = jnp.sum(jnp.where(lane, found[:128], 0.0), axis=0, keepdims=True)
    low = jnp.sum(jnp.where(lane, found[128:], 0.0), axis=0, keepdims=True)
    place = (high * 128.0 + low).astype(jnp.int32)
    shard = lax.broadcasted_iota(jnp.int32, (shards, tok), 0)
    match = (place >= shard * rows_shard) & (place < (shard + 1) * rows_shard)
    matched = jnp.where(match, 1.0, 0.0)
    owner = jnp.sum(jnp.where(match, shard, 0), axis=0, keepdims=True)
    slot = place - owner * rows_shard
    earlier = lax.broadcasted_iota(jnp.int32, (tok, tok), 0) <= lax.broadcasted_iota(
        jnp.int32, (tok, tok), 1
    )
    counts = dot32(matched.astype(bf16), jnp.where(earlier, 1.0, 0.0).astype(bf16))
    rank = jnp.sum(matched * counts, axis=0, keepdims=True).astype(jnp.int32) - 1
    line = lax.broadcasted_iota(jnp.int32, (128, tok), 0)
    spread = jnp.where(line % capacity == rank, 1.0, 0.0).astype(bf16)
    both = (((1,), (1,)), ((), ()))
    codes = [
        lax.dot_general(
            (matched * part.astype(f32)).astype(bf16), spread, both, preferred_element_type=f32
        )
        for part in (slot // 128 + 1, slot % 128)
    ]
    first_half = lax.broadcasted_iota(jnp.int32, (shards, 128), 1) < capacity
    code = jnp.where(first_half, codes[0], codes[1])
    return code, owner * capacity + rank


def pack_kernel(*refs, capacity, rows_shard):
    sources, (out_ref, pos_ref), buffers, sems = refs[:7], refs[7:9], refs[9:16], refs[16]
    copies = [
        pltpu.make_async_copy(source, buffer, sems.at[i])
        for i, (source, buffer) in enumerate(zip(sources, buffers, strict=True))
    ]
    for i in (0, 1, 3, 2, 4, 5, 6):
        copies[i].start()
    for i in (0, 1, 3):
        copies[i].wait()
    cur_ref, prev_ref, grads_ref, places_ref, w_gate_ref, w_up_ref, w_out_ref = buffers
    shards = out_ref.shape[0]
    places = places_ref[...]
    parts = jnp.concatenate(
        [(places // 128).astype(f32), (places % 128).astype(f32)], axis=1
    ).astype(bf16)
    cur_code, cur_pos = packed(cur_ref[...], parts, capacity, shards, rows_shard)
    prev_code, prev_pos = packed(prev_ref[...], parts, capacity, shards, rows_shard)
    pos_ref[...] = cur_pos
    slots = shards * capacity
    slot_row = lax.broadcasted_iota(jnp.int32, (slots, prev_pos.shape[1]), 0)
    pack = jnp.where(slot_row == prev_pos, 1.0, 0.0).astype(bf16)
    for i in (2, 4, 5, 6):
        copies[i].wait()
    rows = dot32(pack, grads_ref[...]).astype(bf16)
    cut = (
        pl.ds(pl.multiple_of((lax.axis_index("x") % 2) * 64, 64), 64),
        pl.ds(pl.multiple_of(lax.axis_index("y") * 128, 128), 128),
    )
    gate_slice = w_gate_ref[cut].astype(f32)
    up_slice = w_up_ref[cut].astype(f32)
    own = jnp.where(lax.axis_index("core") == 0, gate_slice, up_slice).astype(bf16)
    out = jnp.concatenate([w_out_ref[...].astype(f32), jnp.zeros((12, 128), f32)], axis=0)
    tail_row = lax.broadcasted_iota(jnp.int32, (16, 128), 0)
    for shard in range(shards):
        out_ref[shard, :capacity, :] = rows[shard * capacity : (shard + 1) * capacity]
        out_ref[shard, capacity : capacity + 64, :] = own
        tail = jnp.where(tail_row == 14, cur_code[shard : shard + 1], out)
        tail = jnp.where(tail_row == 15, prev_code[shard : shard + 1], tail)
        out_ref[shard, capacity + 64 : capacity + 80, :] = tail.astype(bf16)


def pack(cur_ids, prev_ids, prev_grads, row_place, w_gate, w_up, w_out, shards, capacity, rows_shard):
    vmem = pl.BlockSpec(memory_space=pltpu.VMEM)
    tok = cur_ids.shape[0]
    arrays = (
        cur_ids.reshape(1, tok), prev_ids.reshape(1, tok), prev_grads,
        row_place.reshape(-1, 128), w_gate, w_up, w_out.reshape(4, 128),
    )
    return pl.pallas_call(
        lambda *refs: pack_kernel(*refs, capacity=capacity, rows_shard=rows_shard),
        out_shape=(
            jax.ShapeDtypeStruct((shards, capacity + 80, 128), bf16),
            jax.ShapeDtypeStruct((1, tok), jnp.int32),
        ),
        in_specs=[pl.BlockSpec(memory_space=pltpu.HBM)] * len(arrays),
        out_specs=(vmem, vmem),
        scratch_shapes=[pltpu.VMEM(array.shape, array.dtype) for array in arrays]
        + [pltpu.SemaphoreType.DMA((len(arrays),))],
        compiler_params=pltpu.CompilerParams(vmem_limit_bytes=62 * 1024 * 1024),
        name="pack",
    )(*arrays)


def decoded(line, capacity):
    values = line.astype(jnp.int32)
    return ((values[..., :capacity] - 1) * 128 + values[..., capacity:]).reshape(-1)


def tower_kernel(
    answers_ref, target_ref, own_ref, other_ref, w_gate_ref, w_up_ref, shared_ref,
    gain_ref, labels_ref, table_part_ref, emb_grad_ref, grads_ref, weights_s, gate_s, up_s,
):
    tok = target_ref.shape[1]
    width = answers_ref.shape[1]
    shards, span = shared_ref.shape[:2]
    lines = own_ref.shape[0] // 8
    core = lax.axis_index("core")
    home = lax.axis_index("emb")
    weights_s[core] = own_ref[...]
    weights_s[1 - core] = other_ref[...]
    slot_row = lax.broadcasted_iota(jnp.int32, (answers_ref.shape[0], tok), 0)
    pick = jnp.where(target_ref[...] == slot_row, 1.0, 0.0).astype(bf16)
    values = lax.dot_general(
        pick, answers_ref[...], (((0,), (0,)), ((), ())), preferred_element_type=f32
    )
    turned = labels_ref[...].T
    mine = lax.broadcasted_iota(jnp.int32, turned.shape, 1) == home
    targets = jnp.sum(jnp.where(mine, turned, 0.0), axis=1, keepdims=True)
    inverse_rms = lax.rsqrt(jnp.mean(values * values, axis=1, keepdims=True) + norm_eps)
    gain = gain_ref[...]
    normed_wide = values * inverse_rms * gain
    normed = normed_wide.astype(bf16)
    normed_t = normed_wide.T.astype(bf16)

    turns = (lax.axis_index("x") % 2, 1 - lax.axis_index("x") % 2)

    def far_block(hop, half, side):
        tiles = []
        for tile in (2 * half, 2 * half + 1):
            parts = [
                weights_s[side, pl.ds(pl.multiple_of((tile * 2 + turn) * lines + hop * 64, 64), 64), :]
                for turn in turns
            ]
            tiles.append(jnp.concatenate(parts, axis=0))
        return jnp.concatenate(tiles, axis=1)

    def home_block(hop, half, side):
        return (w_gate_ref, w_up_ref)[side][:, half * 256 : (half + 1) * 256]

    def out_row(shard, half, j):
        return shared_ref[shard, pl.ds(span - 16 + 2 * half + j, 1), :].astype(f32)

    def forward(hop, total, block):
        shard = (home + 1 + hop) % shards
        for half in range(2):
            at = hop * 2 + half
            gate = dot32(normed, block(hop, half, 0))
            up = dot32(normed, block(hop, half, 1))
            sig = jax.nn.sigmoid(gate)
            act = gate * sig
            gate_s[at] = up * (sig + act * (1.0 - sig))
            up_s[at] = act
            hidden = (act * up).astype(bf16).astype(f32)
            for j in range(2):
                total = total + hidden[:, j * 128 : (j + 1) * 128] * out_row(shard, half, j)
        return total

    total = forward(shards - 1, jnp.zeros((tok, 128), f32), home_block)
    total = lax.fori_loop(0, shards - 1, lambda hop, t: forward(hop, t, far_block), total, unroll=True)
    logits = jnp.sum(total, axis=1, keepdims=True)
    slopes = loss_weight * (jax.nn.sigmoid(logits) - targets)

    across = (((1,), (1,)), ((), ()))

    def backward(hop, back, block):
        shard = (home + 1 + hop) % shards
        for half in range(2):
            at = hop * 2 + half
            out = jnp.concatenate([out_row(shard, half, j) for j in range(2)], axis=1)
            back_hidden = slopes * out
            back_gate = (back_hidden * gate_s[at]).astype(bf16)
            back_up = (back_hidden * up_s[at]).astype(bf16)
            for side, part in ((0, back_gate), (1, back_up)):
                back = back + lax.dot_general(
                    part, block(hop, half, side), across, preferred_element_type=f32
                )
                grad = dot32(normed_t, part).astype(bf16)
                place = core if side == 0 else 1 - core
                for j in range(2):
                    tile = 2 * half + j
                    for k in range(4):
                        grads_ref[
                            place, tile * 4 + k, pl.ds(shard * 32, 32), :
                        ] = grad[k * 32 : (k + 1) * 32, j * 128 : (j + 1) * 128]
        return back

    back = backward(shards - 1, jnp.zeros((tok, width), f32), home_block)
    back = lax.fori_loop(0, shards - 1, lambda hop, b: backward(hop, b, far_block), back, unroll=True)
    grads_ref[:, :, shards * 32 :, :] = table_part_ref[...]
    scaled = back * gain
    emb_grad_ref[...] = inverse_rms * scaled - values * (
        inverse_rms * inverse_rms * inverse_rms
    ) * jnp.mean(values * scaled, axis=1, keepdims=True)


def tower(answers, target, own, other, w_gate, w_up, shared, gain, labels, table_part):
    tok = target.shape[1]
    width = answers.shape[1]
    shards = shared.shape[0]
    vmem = pl.BlockSpec(memory_space=pltpu.VMEM)
    return pl.pallas_call(
        tower_kernel,
        out_shape=(
            jax.ShapeDtypeStruct((tok, width), f32),
            jax.ShapeDtypeStruct((2, 16, shards * 32 + table_part.shape[2], width), bf16),
        ),
        in_specs=[vmem] * 10,
        out_specs=(vmem, vmem),
        scratch_shapes=[pltpu.VMEM((2, *own.shape), bf16)]
        + [pltpu.VMEM((2 * shards, tok, 256), f32)] * 2,
        compiler_params=pltpu.CompilerParams(vmem_limit_bytes=20 * 1024 * 1024),
        cost_estimate=pl.CostEstimate(
            flops=6 * 2 * tok * width * 4096, bytes_accessed=5 << 20, transcendentals=2 << 20
        ),
        name="tower",
    )(
        answers, target, own, other, w_gate, w_up, shared,
        gain.reshape(1, -1), labels.reshape(shards, tok), table_part,
    )


def update_kernel(
    own_ref, other_ref, table_ref, accum_ref,
    new_table_ref, new_accum_ref, gate_ref, up_ref, both_s, *, scale,
):
    core = lax.axis_index("core")
    both_s[core] = own_ref[...]
    both_s[1 - core] = other_ref[...]
    plane, lines = own_ref.shape[:2]
    span = lines - 32
    for side, out_ref in ((0, gate_ref), (1, up_ref)):
        for q in range(plane):
            tile, k = q // 4, q % 4
            out_ref[k * 32 : (k + 1) * 32, tile * 128 : (tile + 1) * 128] = (
                both_s[side, q, :32, :].astype(f32) * scale
            )
            rows = pl.ds((2 * q + side) * span, span)
            grad = both_s[side, q, 32:, :].astype(f32)
            total = accum_ref[rows, :] + grad * grad
            new_accum_ref[rows, :] = total
            new_table_ref[rows, :] = table_ref[rows, :] - learn_rate * grad * lax.rsqrt(total)


def update(own, other, table, accum, scale):
    vmem = pl.BlockSpec(memory_space=pltpu.VMEM)
    part = jax.ShapeDtypeStruct((128, 512), f32)
    return pl.pallas_call(
        lambda *refs: update_kernel(*refs, scale=scale),
        out_shape=(
            jax.ShapeDtypeStruct(table.shape, f32),
            jax.ShapeDtypeStruct(table.shape, f32),
            part,
            part,
        ),
        in_specs=[vmem] * 4,
        out_specs=(vmem,) * 4,
        scratch_shapes=[pltpu.VMEM((2, *own.shape), bf16)],
        compiler_params=pltpu.CompilerParams(vmem_limit_bytes=12 * 1024 * 1024),
        name="update",
    )(own, other, table, accum)


def swapped(array, axis):
    return lax.ppermute(array, axis, [(0, 1), (1, 0)])


def step(
    cur_ids, prev_ids, prev_grads, row_place, table, accum, labels, gain, w_gate, w_up, w_out
):
    shards = lax.axis_size("emb")
    plane = lax.axis_size(XY)
    rows_shard, width = table.shape
    tok = cur_ids.shape[0]
    capacity = min(tok, 2 * tok // shards)
    slots = shards * capacity
    core = lax.axis_index("core")
    home = lax.axis_index("emb")
    payload, cur_pos = pack(
        cur_ids, prev_ids, prev_grads, row_place, w_gate, w_up, w_out,
        shards, capacity, rows_shard,
    )
    first = exchange(payload, "emb")
    rows_table = lax.optimization_barrier(table.astype(bf16))
    got_rows = first[:, :capacity].reshape(slots, width)
    slices = first[:, capacity : capacity + 64]
    wanted = decoded(first[:, capacity + 78], capacity)
    got_slots = decoded(first[:, capacity + 79], capacity)

    row_ids = jnp.arange(rows_shard, dtype=jnp.int32)
    hot = (wanted[:, None] == row_ids[None, :]).astype(bf16)
    fetched = dot32(hot, rows_table).astype(bf16)
    span = rows_shard // plane // 2
    half_ids = jnp.arange(rows_shard // 2, dtype=jnp.int32)
    half_ids = half_ids // span * (2 * span) + half_ids % span
    part_ids = jnp.concatenate([half_ids + core * span, half_ids + (1 - core) * span])
    table_part = dot32((part_ids[:, None] == got_slots[None, :]).astype(bf16), got_rows)
    table_part = table_part.astype(bf16).reshape(2, plane, span, width)

    foreign = lax.dynamic_slice(
        jnp.concatenate([slices, slices], axis=0), (home + 1, 0, 0), (shards - 1, 64, 128)
    ).reshape((shards - 1) * 64, 128)
    beside = lax.ppermute(foreign, "x", [(i, i ^ 1) for i in range(lax.axis_size("x"))])
    answers = exchange(fetched.reshape(shards, capacity, width), "emb").reshape(slots, width)
    own_weights = lax.all_gather(
        jnp.concatenate([foreign, beside], axis=0), "y", axis=0, tiled=True
    )
    other_weights = swapped(own_weights, "core")
    emb_grad, tower_grads = tower(
        answers, cur_pos, own_weights, other_weights, w_gate, w_up, first, gain, labels,
        table_part,
    )

    received = swapped(tower_grads[1], "core")
    core_sum = (tower_grads[0].astype(f32) + received.astype(f32)).astype(bf16)
    second = exchange(core_sum, XY)
    plane_sum = second[:, : shards * 32].astype(f32).sum(axis=0).astype(bf16)
    half_grad = second[:, shards * 32 :].astype(f32).sum(axis=0)
    total_grad = (half_grad + swapped(half_grad, "zh")).astype(bf16)
    for_z = jnp.broadcast_to(plane_sum.reshape(1, shards, 32, 128), (2, shards, 32, 128))
    third = exchange(for_z.reshape(2 * shards, 32, 128), ZZ)
    tower_sum = third.astype(f32).sum(axis=0).astype(bf16)
    own = to_all(jnp.concatenate([tower_sum, total_grad], axis=0), XY)
    other = swapped(own, "core")

    tower_scale = 1.0 / math.sqrt(tok * shards * lax.axis_size(DP))
    new_table, new_accum, gate_sum, up_sum = update(own, other, table, accum, tower_scale)
    return (new_table, new_accum, gate_sum, up_sum, emb_grad)


def solution(mesh):
    torus = Mesh(mesh.devices.reshape(4, 4, 2, 2, mesh.shape["emb"]), DP_EMB)
    return jax.shard_map(
        step,
        mesh=torus,
        in_specs=(
            P(DP_EMB),
            P(DP_EMB),
            P(DP_EMB, None),
            P(),
            P("emb", None),
            P("emb", None),
            P(DP),
            P(),
            P(None, "emb"),
            P(None, "emb"),
            P("emb"),
        ),
        out_specs=(P("emb", None), P("emb", None), P(None, "emb"), P(None, "emb"), P(DP_EMB, None)),
        check_vma=False,
    )
```

```python
import math

import jax
import jax.numpy as jnp
from jax import lax
from jax.experimental import pallas as pl
from jax.experimental.pallas import tpu as pltpu
from jax.sharding import Mesh
from jax.sharding import PartitionSpec as P


DP = ("x", "y", "zh", "core")
DP_EMB = ("x", "y", "zh", "core", "emb")
XY = ("x", "y")
ZZ = ("zh", "emb")


loss_weight = 64.0
learn_rate = 0.1
norm_eps = 1e-06

bf16 = jnp.bfloat16
f32 = jnp.float32


def exchange(pieces, axis):
    return lax.all_to_all(pieces, axis, 0, 0, tiled=True)


def to_all(array, axis):
    return exchange(jnp.broadcast_to(array[None], (lax.axis_size(axis), *array.shape)), axis)


def dot32(a, b):
    return jnp.dot(a, b, preferred_element_type=f32)


def packed(ids, parts, capacity, shards, rows_shard):
    tok = ids.shape[1]
    lines = parts.shape[0]
    row = lax.broadcasted_iota(jnp.int32, (lines, tok), 0)
    pick = jnp.where(ids // 128 == row, 1.0, 0.0).astype(bf16)
    found = lax.dot_general(parts, pick, (((0,), (0,)), ((), ())), preferred_element_type=f32)
    lane = lax.broadcasted_iota(jnp.int32, (128, tok), 0) == ids % 128
    high = jnp.sum(jnp.where(lane, found[:128], 0.0), axis=0, keepdims=True)
    low = jnp.sum(jnp.where(lane, found[128:], 0.0), axis=0, keepdims=True)
    place = (high * 128.0 + low).astype(jnp.int32)
    shard = lax.broadcasted_iota(jnp.int32, (shards, tok), 0)
    match = (place >= shard * rows_shard) & (place < (shard + 1) * rows_shard)
    matched = jnp.where(match, 1.0, 0.0)
    owner = jnp.sum(jnp.where(match, shard, 0), axis=0, keepdims=True)
    slot = place - owner * rows_shard
    earlier = lax.broadcasted_iota(jnp.int32, (tok, tok), 0) <= lax.broadcasted_iota(
        jnp.int32, (tok, tok), 1
    )
    counts = dot32(matched.astype(bf16), jnp.where(earlier, 1.0, 0.0).astype(bf16))
    rank = jnp.sum(matched * counts, axis=0, keepdims=True).astype(jnp.int32) - 1
    line = lax.broadcasted_iota(jnp.int32, (128, tok), 0)
    spread = jnp.where(line % capacity == rank, 1.0, 0.0).astype(bf16)
    both = (((1,), (1,)), ((), ()))
    codes = [
        lax.dot_general(
            (matched * part.astype(f32)).astype(bf16), spread, both, preferred_element_type=f32
        )
        for part in (slot // 128 + 1, slot % 128)
    ]
    first_half = lax.broadcasted_iota(jnp.int32, (shards, 128), 1) < capacity
    code = jnp.where(first_half, codes[0], codes[1])
    return code, owner * capacity + rank


def pack_kernel(*refs, capacity, rows_shard):
    sources, (out_ref, pos_ref, sent_ref), buffers, sems = refs[:7], refs[7:10], refs[10:17], refs[17]
    copies = [
        pltpu.make_async_copy(source, buffer, sems.at[i])
        for i, (source, buffer) in enumerate(zip(sources, buffers, strict=True))
    ]
    for i in (0, 1, 3, 2, 4, 5, 6):
        copies[i].start()
    for i in (0, 1, 3):
        copies[i].wait()
    cur_ref, prev_ref, grads_ref, places_ref, w_gate_ref, w_up_ref, w_out_ref = buffers
    shards = out_ref.shape[0]
    places = places_ref[...]
    parts = jnp.concatenate(
        [(places // 128).astype(f32), (places % 128).astype(f32)], axis=1
    ).astype(bf16)
    cur_code, cur_pos = packed(cur_ref[...], parts, capacity, shards, rows_shard)
    prev_code, prev_pos = packed(prev_ref[...], parts, capacity, shards, rows_shard)
    pos_ref[...] = cur_pos
    slots = shards * capacity
    slot_row = lax.broadcasted_iota(jnp.int32, (slots, prev_pos.shape[1]), 0)
    pack = jnp.where(slot_row == prev_pos, 1.0, 0.0).astype(bf16)
    for i in (2, 4, 5, 6):
        copies[i].wait()
    rows = dot32(pack, grads_ref[...]).astype(bf16)
    cut = (
        pl.ds(pl.multiple_of((lax.axis_index("x") % 2) * 64, 64), 64),
        pl.ds(pl.multiple_of(lax.axis_index("y") * 128, 128), 128),
    )
    gate_slice = w_gate_ref[cut].astype(f32)
    up_slice = w_up_ref[cut].astype(f32)
    own = jnp.where(lax.axis_index("core") == 0, gate_slice, up_slice).astype(bf16)
    out = jnp.concatenate([w_out_ref[...].astype(f32), jnp.zeros((12, 128), f32)], axis=0)
    tail_row = lax.broadcasted_iota(jnp.int32, (16, 128), 0)
    for shard in range(shards):
        sent_ref[shard, :capacity, :] = rows[shard * capacity : (shard + 1) * capacity]
        tail = jnp.where(tail_row == 15, prev_code[shard : shard + 1], 0.0)
        sent_ref[shard, capacity : capacity + 16, :] = tail.astype(bf16)
        out_ref[shard, :64, :] = own
        tail = jnp.where(tail_row == 15, cur_code[shard : shard + 1], out)
        out_ref[shard, 64:80, :] = tail.astype(bf16)


def pack(cur_ids, prev_ids, prev_grads, row_place, w_gate, w_up, w_out, shards, capacity, rows_shard):
    vmem = pl.BlockSpec(memory_space=pltpu.VMEM)
    tok = cur_ids.shape[0]
    arrays = (
        cur_ids.reshape(1, tok), prev_ids.reshape(1, tok), prev_grads,
        row_place.reshape(-1, 128), w_gate, w_up, w_out.reshape(4, 128),
    )
    return pl.pallas_call(
        lambda *refs: pack_kernel(*refs, capacity=capacity, rows_shard=rows_shard),
        out_shape=(
            jax.ShapeDtypeStruct((shards, 80, 128), bf16),
            jax.ShapeDtypeStruct((1, tok), jnp.int32),
            jax.ShapeDtypeStruct((shards, capacity + 16, 128), bf16),
        ),
        in_specs=[pl.BlockSpec(memory_space=pltpu.HBM)] * len(arrays),
        out_specs=(vmem, vmem, vmem),
        scratch_shapes=[pltpu.VMEM(array.shape, array.dtype) for array in arrays]
        + [pltpu.SemaphoreType.DMA((len(arrays),))],
        compiler_params=pltpu.CompilerParams(vmem_limit_bytes=62 * 1024 * 1024),
        name="pack",
    )(*arrays)


def decoded(line, capacity):
    values = line.astype(jnp.int32)
    return ((values[..., :capacity] - 1) * 128 + values[..., capacity:]).reshape(-1)


def tower_kernel(
    answers_ref, target_ref, own_ref, other_ref, w_gate_ref, w_up_ref, shared_ref,
    gain_ref, labels_ref, table_part_ref, emb_grad_ref, grads_ref, weights_s, gate_s, up_s,
):
    tok = target_ref.shape[1]
    width = answers_ref.shape[1]
    shards, span = shared_ref.shape[:2]
    lines = own_ref.shape[0] // 8
    core = lax.axis_index("core")
    home = lax.axis_index("emb")
    weights_s[core] = own_ref[...]
    weights_s[1 - core] = other_ref[...]
    slot_row = lax.broadcasted_iota(jnp.int32, (answers_ref.shape[0], tok), 0)
    pick = jnp.where(target_ref[...] == slot_row, 1.0, 0.0).astype(bf16)
    values = lax.dot_general(
        pick, answers_ref[...], (((0,), (0,)), ((), ())), preferred_element_type=f32
    )
    turned = labels_ref[...].T
    mine = lax.broadcasted_iota(jnp.int32, turned.shape, 1) == home
    targets = jnp.sum(jnp.where(mine, turned, 0.0), axis=1, keepdims=True)
    inverse_rms = lax.rsqrt(jnp.mean(values * values, axis=1, keepdims=True) + norm_eps)
    gain = gain_ref[...]
    normed_wide = values * inverse_rms * gain
    normed = normed_wide.astype(bf16)
    normed_t = normed_wide.T.astype(bf16)

    turns = (lax.axis_index("x") % 2, 1 - lax.axis_index("x") % 2)

    def far_block(hop, half, side):
        tiles = []
        for tile in (2 * half, 2 * half + 1):
            parts = [
                weights_s[side, pl.ds(pl.multiple_of((tile * 2 + turn) * lines + hop * 64, 64), 64), :]
                for turn in turns
            ]
            tiles.append(jnp.concatenate(parts, axis=0))
        return jnp.concatenate(tiles, axis=1)

    def home_block(hop, half, side):
        return (w_gate_ref, w_up_ref)[side][:, half * 256 : (half + 1) * 256]

    def out_row(shard, half, j):
        return shared_ref[shard, pl.ds(span - 16 + 2 * half + j, 1), :].astype(f32)

    def forward(hop, total, block):
        shard = (home + 1 + hop) % shards
        for half in range(2):
            at = hop * 2 + half
            gate = dot32(normed, block(hop, half, 0))
            up = dot32(normed, block(hop, half, 1))
            sig = jax.nn.sigmoid(gate)
            act = gate * sig
            gate_s[at] = up * (sig + act * (1.0 - sig))
            up_s[at] = act
            hidden = (act * up).astype(bf16).astype(f32)
            for j in range(2):
                total = total + hidden[:, j * 128 : (j + 1) * 128] * out_row(shard, half, j)
        return total

    total = forward(shards - 1, jnp.zeros((tok, 128), f32), home_block)
    total = lax.fori_loop(0, shards - 1, lambda hop, t: forward(hop, t, far_block), total, unroll=True)
    logits = jnp.sum(total, axis=1, keepdims=True)
    slopes = loss_weight * (jax.nn.sigmoid(logits) - targets)

    across = (((1,), (1,)), ((), ()))

    def backward(hop, back, block):
        shard = (home + 1 + hop) % shards
        for half in range(2):
            at = hop * 2 + half
            out = jnp.concatenate([out_row(shard, half, j) for j in range(2)], axis=1)
            back_hidden = slopes * out
            back_gate = (back_hidden * gate_s[at]).astype(bf16)
            back_up = (back_hidden * up_s[at]).astype(bf16)
            for side, part in ((0, back_gate), (1, back_up)):
                back = back + lax.dot_general(
                    part, block(hop, half, side), across, preferred_element_type=f32
                )
                grad = dot32(normed_t, part).astype(bf16)
                place = core if side == 0 else 1 - core
                for j in range(2):
                    tile = 2 * half + j
                    for k in range(4):
                        grads_ref[
                            place, tile * 4 + k, pl.ds(shard * 32, 32), :
                        ] = grad[k * 32 : (k + 1) * 32, j * 128 : (j + 1) * 128]
        return back

    back = backward(shards - 1, jnp.zeros((tok, width), f32), home_block)
    back = lax.fori_loop(0, shards - 1, lambda hop, b: backward(hop, b, far_block), back, unroll=True)
    grads_ref[:, :, shards * 32 :, :] = table_part_ref[...]
    scaled = back * gain
    emb_grad_ref[...] = inverse_rms * scaled - values * (
        inverse_rms * inverse_rms * inverse_rms
    ) * jnp.mean(values * scaled, axis=1, keepdims=True)


def tower(answers, target, own, other, w_gate, w_up, shared, gain, labels, table_part):
    tok = target.shape[1]
    width = answers.shape[1]
    shards = shared.shape[0]
    vmem = pl.BlockSpec(memory_space=pltpu.VMEM)
    return pl.pallas_call(
        tower_kernel,
        out_shape=(
            jax.ShapeDtypeStruct((tok, width), f32),
            jax.ShapeDtypeStruct((2, 16, shards * 32 + table_part.shape[2], width), bf16),
        ),
        in_specs=[vmem] * 10,
        out_specs=(vmem, vmem),
        scratch_shapes=[pltpu.VMEM((2, *own.shape), bf16)]
        + [pltpu.VMEM((2 * shards, tok, 256), f32)] * 2,
        compiler_params=pltpu.CompilerParams(vmem_limit_bytes=20 * 1024 * 1024),
        cost_estimate=pl.CostEstimate(
            flops=6 * 2 * tok * width * 4096, bytes_accessed=5 << 20, transcendentals=2 << 20
        ),
        name="tower",
    )(
        answers, target, own, other, w_gate, w_up, shared,
        gain.reshape(1, -1), labels.reshape(shards, tok), table_part,
    )


def update_kernel(
    own_ref, other_ref, table_ref, accum_ref,
    new_table_ref, new_accum_ref, gate_ref, up_ref, both_s, *, scale,
):
    core = lax.axis_index("core")
    both_s[core] = own_ref[...]
    both_s[1 - core] = other_ref[...]
    plane, lines = own_ref.shape[:2]
    span = lines - 32
    for side, out_ref in ((0, gate_ref), (1, up_ref)):
        for q in range(plane):
            tile, k = q // 4, q % 4
            out_ref[k * 32 : (k + 1) * 32, tile * 128 : (tile + 1) * 128] = (
                both_s[side, q, :32, :].astype(f32) * scale
            )
            rows = pl.ds((2 * q + side) * span, span)
            grad = both_s[side, q, 32:, :].astype(f32)
            total = accum_ref[rows, :] + grad * grad
            new_accum_ref[rows, :] = total
            new_table_ref[rows, :] = table_ref[rows, :] - learn_rate * grad * lax.rsqrt(total)


def update(own, other, table, accum, scale):
    vmem = pl.BlockSpec(memory_space=pltpu.VMEM)
    part = jax.ShapeDtypeStruct((128, 512), f32)
    return pl.pallas_call(
        lambda *refs: update_kernel(*refs, scale=scale),
        out_shape=(
            jax.ShapeDtypeStruct(table.shape, f32),
            jax.ShapeDtypeStruct(table.shape, f32),
            part,
            part,
        ),
        in_specs=[vmem] * 4,
        out_specs=(vmem,) * 4,
        scratch_shapes=[pltpu.VMEM((2, *own.shape), bf16)],
        compiler_params=pltpu.CompilerParams(vmem_limit_bytes=12 * 1024 * 1024),
        name="update",
    )(own, other, table, accum)


def swapped(array, axis):
    return lax.ppermute(array, axis, [(0, 1), (1, 0)])


def step(
    cur_ids, prev_ids, prev_grads, row_place, table, accum, labels, gain, w_gate, w_up, w_out
):
    shards = lax.axis_size("emb")
    plane = lax.axis_size(XY)
    rows_shard, width = table.shape
    tok = cur_ids.shape[0]
    capacity = min(tok, 2 * tok // shards)
    slots = shards * capacity
    core = lax.axis_index("core")
    home = lax.axis_index("emb")
    payload, cur_pos, prev_payload = pack(
        cur_ids, prev_ids, prev_grads, row_place, w_gate, w_up, w_out,
        shards, capacity, rows_shard,
    )
    first = exchange(payload, "emb")
    rows_table = lax.optimization_barrier(table.astype(bf16))
    slices = first[:, :64]
    wanted = decoded(first[:, 79], capacity)

    row_ids = jnp.arange(rows_shard, dtype=jnp.int32)
    hot = (wanted[:, None] == row_ids[None, :]).astype(bf16)
    fetched = dot32(hot, rows_table).astype(bf16)
    foreign = lax.dynamic_slice(
        jnp.concatenate([slices, slices], axis=0), (home + 1, 0, 0), (shards - 1, 64, 128)
    ).reshape((shards - 1) * 64, 128)
    beside = lax.ppermute(foreign, "x", [(i, i ^ 1) for i in range(lax.axis_size("x"))])
    both = exchange(
        jnp.concatenate([fetched.reshape(shards, capacity, width), prev_payload], axis=1), "emb"
    )
    answers = both[:, :capacity].reshape(slots, width)
    got_rows = both[:, capacity : 2 * capacity].reshape(slots, width)
    got_slots = decoded(both[:, 2 * capacity + 15], capacity)
    own_weights = lax.all_gather(
        jnp.concatenate([foreign, beside], axis=0), "y", axis=0, tiled=True
    )
    other_weights = swapped(own_weights, "core")
    span = rows_shard // plane // 2
    half_ids = jnp.arange(rows_shard // 2, dtype=jnp.int32)
    half_ids = half_ids // span * (2 * span) + half_ids % span
    part_ids = jnp.concatenate([half_ids + core * span, half_ids + (1 - core) * span])
    table_part = dot32((part_ids[:, None] == got_slots[None, :]).astype(bf16), got_rows)
    table_part = table_part.astype(bf16).reshape(2, plane, span, width)

    emb_grad, tower_grads = tower(
        answers, cur_pos, own_weights, other_weights, w_gate, w_up, first, gain, labels,
        table_part,
    )

    received = swapped(tower_grads[1], "core")
    core_sum = (tower_grads[0].astype(f32) + received.astype(f32)).astype(bf16)
    second = exchange(core_sum, XY)
    plane_sum = second[:, : shards * 32].astype(f32).sum(axis=0).astype(bf16)
    half_grad = second[:, shards * 32 :].astype(f32).sum(axis=0)
    total_grad = (half_grad + swapped(half_grad, "zh")).astype(bf16)
    for_z = jnp.broadcast_to(plane_sum.reshape(1, shards, 32, 128), (2, shards, 32, 128))
    third = exchange(for_z.reshape(2 * shards, 32, 128), ZZ)
    tower_sum = third.astype(f32).sum(axis=0).astype(bf16)
    own = to_all(jnp.concatenate([tower_sum, total_grad], axis=0), XY)
    other = swapped(own, "core")

    tower_scale = 1.0 / math.sqrt(tok * shards * lax.axis_size(DP))
    new_table, new_accum, gate_sum, up_sum = update(own, other, table, accum, tower_scale)
    return (new_table, new_accum, gate_sum, up_sum, emb_grad)


def solution(mesh):
    torus = Mesh(mesh.devices.reshape(4, 4, 2, 2, mesh.shape["emb"]), DP_EMB)
    return jax.shard_map(
        step,
        mesh=torus,
        in_specs=(
            P(DP_EMB),
            P(DP_EMB),
            P(DP_EMB, None),
            P(),
            P("emb", None),
            P("emb", None),
            P(DP),
            P(),
            P(None, "emb"),
            P(None, "emb"),
            P("emb"),
        ),
        out_specs=(P("emb", None), P("emb", None), P(None, "emb"), P(None, "emb"), P(DP_EMB, None)),
        check_vma=False,
    )
```

```python
import math

import jax
import jax.numpy as jnp
from jax import lax
from jax.experimental import pallas as pl
from jax.experimental.pallas import tpu as pltpu
from jax.sharding import Mesh
from jax.sharding import PartitionSpec as P


DP = ("x", "y", "zh", "core")
DP_EMB = ("x", "y", "zh", "core", "emb")
XY = ("x", "y")
ZZ = ("zh", "emb")


loss_weight = 64.0
learn_rate = 0.1
norm_eps = 1e-06

bf16 = jnp.bfloat16
f32 = jnp.float32


def exchange(pieces, axis):
    return lax.all_to_all(pieces, axis, 0, 0, tiled=True)


def to_all(array, axis):
    return exchange(jnp.broadcast_to(array[None], (lax.axis_size(axis), *array.shape)), axis)


def dot32(a, b):
    return jnp.dot(a, b, preferred_element_type=f32)


def packed(ids, parts, capacity, shards, rows_shard):
    tok = ids.shape[1]
    lines = parts.shape[0]
    row = lax.broadcasted_iota(jnp.int32, (lines, tok), 0)
    pick = jnp.where(ids // 128 == row, 1.0, 0.0).astype(bf16)
    found = lax.dot_general(parts, pick, (((0,), (0,)), ((), ())), preferred_element_type=f32)
    lane = lax.broadcasted_iota(jnp.int32, (128, tok), 0) == ids % 128
    high = jnp.sum(jnp.where(lane, found[:128], 0.0), axis=0, keepdims=True)
    low = jnp.sum(jnp.where(lane, found[128:], 0.0), axis=0, keepdims=True)
    place = (high * 128.0 + low).astype(jnp.int32)
    shard = lax.broadcasted_iota(jnp.int32, (shards, tok), 0)
    match = (place >= shard * rows_shard) & (place < (shard + 1) * rows_shard)
    matched = jnp.where(match, 1.0, 0.0)
    owner = jnp.sum(jnp.where(match, shard, 0), axis=0, keepdims=True)
    slot = place - owner * rows_shard
    earlier = lax.broadcasted_iota(jnp.int32, (tok, tok), 0) <= lax.broadcasted_iota(
        jnp.int32, (tok, tok), 1
    )
    counts = dot32(matched.astype(bf16), jnp.where(earlier, 1.0, 0.0).astype(bf16))
    rank = jnp.sum(matched * counts, axis=0, keepdims=True).astype(jnp.int32) - 1
    line = lax.broadcasted_iota(jnp.int32, (128, tok), 0)
    spread = jnp.where(line % capacity == rank, 1.0, 0.0).astype(bf16)
    both = (((1,), (1,)), ((), ()))
    codes = [
        lax.dot_general(
            (matched * part.astype(f32)).astype(bf16), spread, both, preferred_element_type=f32
        )
        for part in (slot // 128 + 1, slot % 128)
    ]
    first_half = lax.broadcasted_iota(jnp.int32, (shards, 128), 1) < capacity
    code = jnp.where(first_half, codes[0], codes[1])
    return code, owner * capacity + rank


def pack_kernel(*refs, capacity, rows_shard):
    sources, (out_ref, pos_ref, sent_ref), buffers, sems = refs[:7], refs[7:10], refs[10:17], refs[17]
    copies = [
        pltpu.make_async_copy(source, buffer, sems.at[i])
        for i, (source, buffer) in enumerate(zip(sources, buffers, strict=True))
    ]
    for i in (0, 1, 3, 2, 4, 5, 6):
        copies[i].start()
    for i in (0, 1, 3):
        copies[i].wait()
    cur_ref, prev_ref, grads_ref, places_ref, w_gate_ref, w_up_ref, w_out_ref = buffers
    shards = out_ref.shape[0]
    places = places_ref[...]
    parts = jnp.concatenate(
        [(places // 128).astype(f32), (places % 128).astype(f32)], axis=1
    ).astype(bf16)
    cur_code, cur_pos = packed(cur_ref[...], parts, capacity, shards, rows_shard)
    prev_code, prev_pos = packed(prev_ref[...], parts, capacity, shards, rows_shard)
    pos_ref[...] = cur_pos
    slots = shards * capacity
    slot_row = lax.broadcasted_iota(jnp.int32, (slots, prev_pos.shape[1]), 0)
    pack = jnp.where(slot_row == prev_pos, 1.0, 0.0).astype(bf16)
    for i in (2, 4, 5, 6):
        copies[i].wait()
    rows = dot32(pack, grads_ref[...]).astype(bf16)
    cut = (
        pl.ds(pl.multiple_of((lax.axis_index("x") % 2) * 64, 64), 64),
        pl.ds(pl.multiple_of(lax.axis_index("y") * 128, 128), 128),
    )
    gate_slice = w_gate_ref[cut].astype(f32)
    up_slice = w_up_ref[cut].astype(f32)
    own = jnp.where(lax.axis_index("core") == 0, gate_slice, up_slice).astype(bf16)
    out = jnp.concatenate([w_out_ref[...].astype(f32), jnp.zeros((12, 128), f32)], axis=0)
    tail_row = lax.broadcasted_iota(jnp.int32, (16, 128), 0)
    for shard in range(shards):
        sent_ref[shard, :capacity, :] = rows[shard * capacity : (shard + 1) * capacity]
        tail = jnp.where(tail_row == 15, prev_code[shard : shard + 1], 0.0)
        sent_ref[shard, capacity : capacity + 16, :] = tail.astype(bf16)
        out_ref[shard, :64, :] = own
        tail = jnp.where(tail_row == 15, cur_code[shard : shard + 1], out)
        out_ref[shard, 64:80, :] = tail.astype(bf16)


def pack(cur_ids, prev_ids, prev_grads, row_place, w_gate, w_up, w_out, shards, capacity, rows_shard):
    vmem = pl.BlockSpec(memory_space=pltpu.VMEM)
    tok = cur_ids.shape[0]
    arrays = (
        cur_ids.reshape(1, tok), prev_ids.reshape(1, tok), prev_grads,
        row_place.reshape(-1, 128), w_gate, w_up, w_out.reshape(4, 128),
    )
    return pl.pallas_call(
        lambda *refs: pack_kernel(*refs, capacity=capacity, rows_shard=rows_shard),
        out_shape=(
            jax.ShapeDtypeStruct((shards, 80, 128), bf16),
            jax.ShapeDtypeStruct((1, tok), jnp.int32),
            jax.ShapeDtypeStruct((shards, capacity + 16, 128), bf16),
        ),
        in_specs=[pl.BlockSpec(memory_space=pltpu.HBM)] * len(arrays),
        out_specs=(vmem, vmem, vmem),
        scratch_shapes=[pltpu.VMEM(array.shape, array.dtype) for array in arrays]
        + [pltpu.SemaphoreType.DMA((len(arrays),))],
        compiler_params=pltpu.CompilerParams(vmem_limit_bytes=62 * 1024 * 1024),
        name="pack",
    )(*arrays)


def decoded(line, capacity):
    values = line.astype(jnp.int32)
    return ((values[..., :capacity] - 1) * 128 + values[..., capacity:]).reshape(-1)


def tower_kernel(
    answers_ref, target_ref, own_ref, other_ref, w_gate_ref, w_up_ref, shared_ref,
    gain_ref, labels_ref, table_part_ref, emb_grad_ref, grads_ref, weights_s, gate_s, up_s,
):
    tok = target_ref.shape[1]
    width = answers_ref.shape[1]
    shards, span = shared_ref.shape[:2]
    lines = own_ref.shape[0] // 8
    core = lax.axis_index("core")
    home = lax.axis_index("emb")
    weights_s[core] = own_ref[...]
    weights_s[1 - core] = other_ref[...]
    slot_row = lax.broadcasted_iota(jnp.int32, (answers_ref.shape[0], tok), 0)
    pick = jnp.where(target_ref[...] == slot_row, 1.0, 0.0).astype(bf16)
    values = lax.dot_general(
        pick, answers_ref[...], (((0,), (0,)), ((), ())), preferred_element_type=f32
    )
    turned = labels_ref[...].T
    mine = lax.broadcasted_iota(jnp.int32, turned.shape, 1) == home
    targets = jnp.sum(jnp.where(mine, turned, 0.0), axis=1, keepdims=True)
    inverse_rms = lax.rsqrt(jnp.mean(values * values, axis=1, keepdims=True) + norm_eps)
    gain = gain_ref[...]
    normed_wide = values * inverse_rms * gain
    normed = normed_wide.astype(bf16)
    normed_t = normed_wide.T.astype(bf16)

    turns = (lax.axis_index("x") % 2, 1 - lax.axis_index("x") % 2)

    def far_block(hop, half, side):
        tiles = []
        for tile in (2 * half, 2 * half + 1):
            parts = [
                weights_s[side, pl.ds(pl.multiple_of((tile * 2 + turn) * lines + hop * 64, 64), 64), :]
                for turn in turns
            ]
            tiles.append(jnp.concatenate(parts, axis=0))
        return jnp.concatenate(tiles, axis=1)

    def home_block(hop, half, side):
        return (w_gate_ref, w_up_ref)[side][:, half * 256 : (half + 1) * 256]

    def out_row(shard, half, j):
        return shared_ref[shard, pl.ds(span - 16 + 2 * half + j, 1), :].astype(f32)

    def forward(hop, total, block):
        shard = (home + 1 + hop) % shards
        for half in range(2):
            at = hop * 2 + half
            gate = dot32(normed, block(hop, half, 0))
            up = dot32(normed, block(hop, half, 1))
            sig = jax.nn.sigmoid(gate)
            act = gate * sig
            gate_s[at] = up * (sig + act * (1.0 - sig))
            up_s[at] = act
            hidden = (act * up).astype(bf16).astype(f32)
            for j in range(2):
                total = total + hidden[:, j * 128 : (j + 1) * 128] * out_row(shard, half, j)
        return total

    total = forward(shards - 1, jnp.zeros((tok, 128), f32), home_block)
    total = lax.fori_loop(0, shards - 1, lambda hop, t: forward(hop, t, far_block), total, unroll=True)
    logits = jnp.sum(total, axis=1, keepdims=True)
    slopes = loss_weight * (jax.nn.sigmoid(logits) - targets)

    across = (((1,), (1,)), ((), ()))

    def backward(hop, back, block):
        shard = (home + 1 + hop) % shards
        for half in range(2):
            at = hop * 2 + half
            out = jnp.concatenate([out_row(shard, half, j) for j in range(2)], axis=1)
            back_hidden = slopes * out
            back_gate = (back_hidden * gate_s[at]).astype(bf16)
            back_up = (back_hidden * up_s[at]).astype(bf16)
            for side, part in ((0, back_gate), (1, back_up)):
                back = back + lax.dot_general(
                    part, block(hop, half, side), across, preferred_element_type=f32
                )
                grad = dot32(normed_t, part).astype(bf16)
                place = core if side == 0 else 1 - core
                for j in range(2):
                    tile = 2 * half + j
                    for k in range(4):
                        grads_ref[
                            place, tile * 4 + k, pl.ds(shard * 32, 32), :
                        ] = grad[k * 32 : (k + 1) * 32, j * 128 : (j + 1) * 128]
        return back

    back = backward(shards - 1, jnp.zeros((tok, width), f32), home_block)
    back = lax.fori_loop(0, shards - 1, lambda hop, b: backward(hop, b, far_block), back, unroll=True)
    grads_ref[:, :, shards * 32 :, :] = table_part_ref[...]
    scaled = back * gain
    emb_grad_ref[...] = inverse_rms * scaled - values * (
        inverse_rms * inverse_rms * inverse_rms
    ) * jnp.mean(values * scaled, axis=1, keepdims=True)


def tower(answers, target, own, other, w_gate, w_up, shared, gain, labels, table_part):
    tok = target.shape[1]
    width = answers.shape[1]
    shards = shared.shape[0]
    vmem = pl.BlockSpec(memory_space=pltpu.VMEM)
    return pl.pallas_call(
        tower_kernel,
        out_shape=(
            jax.ShapeDtypeStruct((tok, width), f32),
            jax.ShapeDtypeStruct((2, 16, shards * 32 + table_part.shape[2], width), bf16),
        ),
        in_specs=[vmem] * 10,
        out_specs=(vmem, vmem),
        scratch_shapes=[pltpu.VMEM((2, *own.shape), bf16)]
        + [pltpu.VMEM((2 * shards, tok, 256), f32)] * 2,
        compiler_params=pltpu.CompilerParams(vmem_limit_bytes=20 * 1024 * 1024),
        cost_estimate=pl.CostEstimate(
            flops=6 * 2 * tok * width * 4096, bytes_accessed=5 << 20, transcendentals=2 << 20
        ),
        name="tower",
    )(
        answers, target, own, other, w_gate, w_up, shared,
        gain.reshape(1, -1), labels.reshape(shards, tok), table_part,
    )


def update_kernel(
    own_ref, other_ref, table_ref, accum_ref,
    new_table_ref, new_accum_ref, gate_ref, up_ref, both_s, *, scale,
):
    core = lax.axis_index("core")
    both_s[core] = own_ref[...]
    both_s[1 - core] = other_ref[...]
    plane, lines = own_ref.shape[:2]
    span = lines - 32
    for side, out_ref in ((0, gate_ref), (1, up_ref)):
        for q in range(plane):
            tile, k = q // 4, q % 4
            out_ref[k * 32 : (k + 1) * 32, tile * 128 : (tile + 1) * 128] = (
                both_s[side, q, :32, :].astype(f32) * scale
            )
            rows = pl.ds((2 * q + side) * span, span)
            grad = both_s[side, q, 32:, :].astype(f32)
            total = accum_ref[rows, :] + grad * grad
            new_accum_ref[rows, :] = total
            new_table_ref[rows, :] = table_ref[rows, :] - learn_rate * grad * lax.rsqrt(total)


def update(own, other, table, accum, scale):
    vmem = pl.BlockSpec(memory_space=pltpu.VMEM)
    part = jax.ShapeDtypeStruct((128, 512), f32)
    return pl.pallas_call(
        lambda *refs: update_kernel(*refs, scale=scale),
        out_shape=(
            jax.ShapeDtypeStruct(table.shape, f32),
            jax.ShapeDtypeStruct(table.shape, f32),
            part,
            part,
        ),
        in_specs=[vmem] * 4,
        out_specs=(vmem,) * 4,
        scratch_shapes=[pltpu.VMEM((2, *own.shape), bf16)],
        compiler_params=pltpu.CompilerParams(vmem_limit_bytes=12 * 1024 * 1024),
        name="update",
    )(own, other, table, accum)


def swapped(array, axis):
    return lax.ppermute(array, axis, [(0, 1), (1, 0)])


def step(
    cur_ids, prev_ids, prev_grads, row_place, table, accum, labels, gain, w_gate, w_up, w_out
):
    shards = lax.axis_size("emb")
    plane = lax.axis_size(XY)
    rows_shard, width = table.shape
    tok = cur_ids.shape[0]
    capacity = min(tok, 2 * tok // shards)
    slots = shards * capacity
    core = lax.axis_index("core")
    home = lax.axis_index("emb")
    payload, cur_pos, prev_payload = pack(
        cur_ids, prev_ids, prev_grads, row_place, w_gate, w_up, w_out,
        shards, capacity, rows_shard,
    )
    first = exchange(payload, "emb")
    rows_table = lax.optimization_barrier(table.astype(bf16))
    slices = first[:, :64]
    wanted = decoded(first[:, 79], capacity)

    row_ids = jnp.arange(rows_shard, dtype=jnp.int32)
    hot = (wanted[:, None] == row_ids[None, :]).astype(bf16)
    fetched = dot32(hot, rows_table).astype(bf16)
    foreign = lax.dynamic_slice(
        jnp.concatenate([slices, slices], axis=0), (home + 1, 0, 0), (shards - 1, 64, 128)
    ).reshape((shards - 1) * 64, 128)
    beside = lax.ppermute(foreign, "x", [(i, i ^ 1) for i in range(lax.axis_size("x"))])
    both = exchange(
        jnp.concatenate([fetched.reshape(shards, capacity, width), prev_payload], axis=1), "emb"
    )
    answers = both[:, :capacity].reshape(slots, width)
    got_rows = both[:, capacity : 2 * capacity].reshape(slots, width)
    got_slots = decoded(both[:, 2 * capacity + 15], capacity)
    own_weights = lax.all_gather(
        jnp.concatenate([foreign, beside], axis=0), "y", axis=0, tiled=True
    )
    other_weights = swapped(own_weights, "core")
    span = rows_shard // plane // 2
    half_ids = jnp.arange(rows_shard // 2, dtype=jnp.int32)
    half_ids = half_ids // span * (2 * span) + half_ids % span
    part_ids = jnp.concatenate([half_ids + core * span, half_ids + (1 - core) * span])
    table_part = dot32((part_ids[:, None] == got_slots[None, :]).astype(bf16), got_rows)
    table_part = table_part.astype(bf16).reshape(2, plane, span, width)

    emb_grad, tower_grads = tower(
        answers, cur_pos, own_weights, other_weights, w_gate, w_up, first, gain, labels,
        table_part,
    )

    received = swapped(tower_grads[1], "core")
    core_sum = (tower_grads[0].astype(f32) + received.astype(f32)).astype(bf16)
    second = exchange(core_sum, XY)
    plane_sum = second[:, : shards * 32].astype(f32).sum(axis=0).astype(bf16)
    half_grad = second[:, shards * 32 :].astype(f32).sum(axis=0).astype(bf16)
    for_z = jnp.concatenate(
        [
            plane_sum.reshape(shards, 32, 128),
            jnp.broadcast_to(half_grad[None], (shards, *half_grad.shape)),
        ],
        axis=1,
    )
    for_z = jnp.broadcast_to(for_z[None], (2, *for_z.shape)).reshape(2 * shards, *for_z.shape[1:])
    third = exchange(for_z, ZZ)
    tower_sum = third[:, :32].astype(f32).sum(axis=0).astype(bf16)
    halves = third[:, 32:].reshape(2, shards, *half_grad.shape)
    halves = lax.dynamic_index_in_dim(halves, home, 1, keepdims=False).astype(f32)
    total_grad = (halves[0] + halves[1]).astype(bf16)
    own = to_all(jnp.concatenate([tower_sum, total_grad], axis=0), XY)
    other = swapped(own, "core")

    tower_scale = 1.0 / math.sqrt(tok * shards * lax.axis_size(DP))
    new_table, new_accum, gate_sum, up_sum = update(own, other, table, accum, tower_scale)
    return (new_table, new_accum, gate_sum, up_sum, emb_grad)


def solution(mesh):
    torus = Mesh(mesh.devices.reshape(4, 4, 2, 2, mesh.shape["emb"]), DP_EMB)
    return jax.shard_map(
        step,
        mesh=torus,
        in_specs=(
            P(DP_EMB),
            P(DP_EMB),
            P(DP_EMB, None),
            P(),
            P("emb", None),
            P("emb", None),
            P(DP),
            P(),
            P(None, "emb"),
            P(None, "emb"),
            P("emb"),
        ),
        out_specs=(P("emb", None), P("emb", None), P(None, "emb"), P(None, "emb"), P(DP_EMB, None)),
        check_vma=False,
    )
```
